1024 devices in a mesh: patch: 2 (over core), theta: 32 (over z), phi: 16 (over x, y).
Axes of the slice: x: 4, y: 4, z: 32, core: 2. Of those that a mesh axis runs over, the one named last changes fastest.
Arguments:
- density: float32 [2, 16, 512, 2048], P('patch', None, 'theta', 'phi'), may hold values from 0.5 to 2
- velocity: float32 [2, 3, 16, 512, 2048], P('patch', None, None, 'theta', 'phi'), may hold values from -3 to 3
- magnetic: float32 [2, 3, 16, 512, 2048], P('patch', None, None, 'theta', 'phi'), may hold values from -3 to 3
- pressure: float32 [2, 16, 512, 2048], P('patch', None, 'theta', 'phi'), may hold values from 0.5 to 2
- send_row: int32 [2, 32, 16, 96], P('patch', 'theta', 'phi'), may hold values from 0 to 14
- send_col: int32 [2, 32, 16, 96], P('patch', 'theta', 'phi'), may hold values from 0 to 126
- send_weight: float32 [2, 32, 16, 2, 96], P('patch', 'theta', 'phi'), may hold values from 0 to 1
- send_turn: float32 [2, 32, 16, 96], P('patch', 'theta', 'phi'), may hold values from -3.140625 to 3.140625
- send_dest: int32 [2, 32, 16, 96], P('patch', 'theta', 'phi'), may hold values from 0 to 5120, as said below
Outputs:
- new_density: float32 [2, 16, 512, 2048], P('patch', None, 'theta', 'phi')
- new_velocity: float32 [2, 3, 16, 512, 2048], P('patch', None, None, 'theta', 'phi')
- new_magnetic: float32 [2, 3, 16, 512, 2048], P('patch', None, None, 'theta', 'phi')
- new_pressure: float32 [2, 16, 512, 2048], P('patch', None, 'theta', 'phi')
The draws below stay inside these ranges and needn't reach their ends.
Inputs may be any that keep to these rules, and one draw needn't show every extreme that they name: `send_dest`: each ghost point m < 5120 of a patch is named by exactly one slot of the other patch's tiles; unused slots hold 5120. Used slots lie only in tiles of the first and last tile rows and tile columns of a patch, and their donor cells lie within min(16, 128) cells of the patch's outer edge; the four corner tiles use all 96 slots, every other tile fewer.
All inputs are finite; a program needn't handle non-finite values.
Results may differ from the reference program's by a relative error of at most 0.00008.
Values sent between devices are 32-bit elements; how exact they have to be, the bound alone decides.
A program may use at most 32 MiB of HBM per device.

```python
import math
import jax
import jax.numpy as jnp
from jax import lax

NR = 16
CT = 16
CP = 128
NTH = 512
NPH = 2048
BORDER = 5120
SEND = 96
N_THETA = 32
N_PHI = 16


def donor_layout(key):
    row_tiles = NTH // CT
    col_tiles = NPH // CP
    tile_count = row_tiles * col_tiles
    slot_count = tile_count * SEND

    def one_patch(patch_key):
        inset_key, order_key, row_key, col_key = jax.random.split(patch_key, 4)
        ghost = jnp.arange(BORDER, dtype=jnp.int32)
        side = jnp.where(ghost < NPH, 0, jnp.where(ghost < 2 * NPH, 1, jnp.where(ghost < 2 * NPH + NTH, 2, 3)))
        offset = jnp.where(side == 0, 0, jnp.where(side == 1, NPH, jnp.where(side == 2, 2 * NPH, 2 * NPH + NTH)))
        along = ghost - offset
        depth = jax.random.randint(inset_key, (BORDER,), 0, min(CT, CP) - 1, dtype=jnp.int32)
        down_row = jnp.minimum(along * NTH // NPH, NTH - 2)
        up_row = jnp.minimum(jnp.maximum(NPH - 1 - along, 0) * NTH // NPH, NTH - 2)
        fwd_col = jnp.minimum(along * NPH // NTH, NPH - 2)
        back_col = jnp.minimum(jnp.maximum(NTH - 1 - along, 0) * NPH // NTH, NPH - 2)
        row_cell = jnp.where(side == 0, down_row, jnp.where(side == 1, up_row, jnp.where(side == 2, depth, NTH - 2 - depth)))
        col_cell = jnp.where(side == 0, depth, jnp.where(side == 1, NPH - 2 - depth, jnp.where(side == 2, fwd_col, back_col)))
        tile_row = row_cell // CT
        tile_col = col_cell // CP
        local_row = jnp.minimum(row_cell - tile_row * CT, CT - 2)
        local_col = jnp.minimum(col_cell - tile_col * CP, CP - 2)
        tile = tile_row * col_tiles + tile_col
        priority = jax.random.permutation(order_key, BORDER).astype(jnp.int32)
        order = jnp.argsort(tile * BORDER + priority, stable=True).astype(jnp.int32)
        sorted_tile = tile[order]
        counts = jnp.zeros((tile_count,), jnp.int32).at[tile].add(1)
        starts = jnp.cumsum(counts).astype(jnp.int32) - counts
        slot = jnp.arange(BORDER, dtype=jnp.int32) - starts[sorted_tile]
        flat = sorted_tile * SEND + slot
        target = jnp.full((slot_count,), BORDER, dtype=jnp.int32).at[flat].set(order)
        rows = jax.random.randint(row_key, (slot_count,), 0, CT - 1, dtype=jnp.int32).at[flat].set(local_row[order])
        cols = jax.random.randint(col_key, (slot_count,), 0, CP - 1, dtype=jnp.int32).at[flat].set(local_col[order])
        shape = (row_tiles, col_tiles, SEND)
        return (target.reshape(shape), rows.reshape(shape), cols.reshape(shape))
    first = one_patch(jax.random.fold_in(key, 11))
    second = one_patch(jax.random.fold_in(key, 23))
    return (jnp.stack([first[0], second[0]]), jnp.stack([first[1], second[1]]), jnp.stack([first[2], second[2]]))


def draw_send_dest(key, part):
    return donor_layout(key)[0]


def draw_send_row(key, part):
    return donor_layout(key)[1]


def draw_send_col(key, part):
    return donor_layout(key)[2]


def steps_of(own_key, extent, cuts, low, top_value):
    loudness, own = 1.0, jax.random.fold_in(own_key, 6)
    for dim, shards_of in cuts:
        heights = jnp.exp(jax.random.uniform(jax.random.fold_in(own, dim), (shards_of,), jnp.float32, low / len(cuts), top_value / len(cuts)))
        loudness = loudness * jnp.repeat(heights, extent[dim] // shards_of).reshape([-1 if axis == dim else 1 for axis in range(len(extent))])
    return loudness


def gaussian(rng, extent, deviation, most, cuts=(), kind=jnp.bfloat16):
    entries = deviation * jax.random.normal(rng, extent, jnp.float32)
    if cuts:
        entries = entries * steps_of(rng, extent, cuts, -0.22, 0.18)
    return jnp.clip(entries, -most, most).astype(kind)


def setup_inputs(seed: int = 0) -> dict:
    splits = jax.random.split(jax.random.key(seed), 10)
    return {
        "density": jnp.clip(jnp.exp(math.log(2.0) - 1.3862944 * jax.random.uniform(splits[0], (2, NR, NTH, NPH), jnp.float32) ** steps_of(splits[0], (2, NR, NTH, NPH), ((0, 2), (2, 32), (3, 16)), -0.2, 0.2)), 0.5, 2.0),
        "velocity": gaussian(splits[1], (2, 3, NR, NTH, NPH), 0.5, 3.0, ((0, 2), (3, 32), (4, 16)), jnp.float32),
        "magnetic": gaussian(splits[2], (2, 3, NR, NTH, NPH), 0.5, 3.0, ((0, 2), (3, 32), (4, 16)), jnp.float32),
        "pressure": jnp.clip(jnp.exp(math.log(2.0) - 1.3862944 * jax.random.uniform(splits[3], (2, NR, NTH, NPH), jnp.float32) ** steps_of(splits[3], (2, NR, NTH, NPH), ((0, 2), (2, 32), (3, 16)), -0.2, 0.2)), 0.5, 2.0),
        "send_row": draw_send_row(jax.random.fold_in(splits[9], 71), 0),
        "send_col": draw_send_col(jax.random.fold_in(splits[9], 71), 0),
        "send_weight": jnp.clip(1.0 * jax.random.uniform(splits[6], (2, N_THETA, N_PHI, 2, SEND), jnp.float32) ** steps_of(splits[6], (2, N_THETA, N_PHI, 2, SEND), ((0, 2), (1, 32), (2, 16)), -0.2, 0.2), 0.0, 1.0),
        "send_turn": jnp.clip(jax.random.uniform(splits[7], (2, N_THETA, N_PHI, SEND), jnp.float32, -3.140625, 3.140625), -3.140625, 3.140625),
        "send_dest": draw_send_dest(jax.random.fold_in(splits[9], 71), 0),
    }


GAMMA = 5.0 / 3.0
R_BASE = 0.6
DR_STEP = 0.65 / 64.0
COURANT = 0.4
DIFFUSE = 0.4


def grid_constants(total_theta, total_phi):
    d_theta = 0.5 * math.pi / total_theta
    d_phi = 1.5 * math.pi / total_phi
    r_low = R_BASE + 0.5 * DR_STEP
    inv_r = 1.0 / DR_STEP
    inv_t = 1.0 / (r_low * d_theta)
    inv_p = 1.0 / (r_low * math.sin(0.25 * math.pi) * d_phi)
    dt_step = COURANT / (inv_r + inv_t + inv_p)
    diffusivity = DIFFUSE / (dt_step * (inv_r * inv_r + inv_t * inv_t + inv_p * inv_p))
    return d_theta, d_phi, dt_step, diffusivity


def bilinear(low_low, low_high, high_low, high_high, weight_row, weight_col):
    return (1.0 - weight_row) * ((1.0 - weight_col) * low_low + weight_col * low_high) + weight_row * ((1.0 - weight_col) * high_low + weight_col * high_high)


def turn_frame(blended, turn):
    cos_t = jnp.cos(turn)
    sin_t = jnp.sin(turn)
    flow_t = cos_t * blended[2] + sin_t * blended[3]
    flow_p = cos_t * blended[3] - sin_t * blended[2]
    field_t = cos_t * blended[5] + sin_t * blended[6]
    field_p = cos_t * blended[6] - sin_t * blended[5]
    return jnp.stack([blended[0], blended[1], flow_t, flow_p, blended[4], field_t, field_p, blended[7]])


def advance(padded, radius, sin_theta, d_theta, d_phi, dt_step, diffusivity):
    levels = padded.shape[1] - 2
    tile_rows = padded.shape[2] - 2
    tile_cols = padded.shape[3] - 2
    radial_h = 1.0 / DR_STEP
    colat_h = 1.0 / (radius[:, None, None] * d_theta)
    lon_h = 1.0 / (radius[:, None, None] * sin_theta[None, :, None] * d_phi)

    def shifted(field, step_r, step_t, step_p):
        return field[..., 1 + step_r:1 + step_r + levels, 1 + step_t:1 + step_t + tile_rows, 1 + step_p:1 + step_p + tile_cols]

    def radial_diff(field):
        return (shifted(field, 1, 0, 0) - shifted(field, -1, 0, 0)) * (0.5 * radial_h)

    def colat_diff(field):
        return (shifted(field, 0, 1, 0) - shifted(field, 0, -1, 0)) * (0.5 * colat_h)

    def lon_diff(field):
        return (shifted(field, 0, 0, 1) - shifted(field, 0, 0, -1)) * (0.5 * lon_h)

    def laplace(field):
        centre = 2.0 * shifted(field, 0, 0, 0)
        return ((shifted(field, 1, 0, 0) + shifted(field, -1, 0, 0) - centre) * (radial_h * radial_h)
                + (shifted(field, 0, 1, 0) + shifted(field, 0, -1, 0) - centre) * (colat_h * colat_h)
                + (shifted(field, 0, 0, 1) + shifted(field, 0, 0, -1) - centre) * (lon_h * lon_h))

    def cross_of(left_vec, right_vec):
        return jnp.stack([left_vec[1] * right_vec[2] - left_vec[2] * right_vec[1],
                          left_vec[2] * right_vec[0] - left_vec[0] * right_vec[2],
                          left_vec[0] * right_vec[1] - left_vec[1] * right_vec[0]])

    def curl_of(field):
        return jnp.stack([colat_diff(field[2]) - lon_diff(field[1]),
                          lon_diff(field[0]) - radial_diff(field[2]),
                          radial_diff(field[1]) - colat_diff(field[0])])

    density_pad = padded[0]
    flow_pad = padded[1:4]
    magnet_pad = padded[4:7]
    press_pad = padded[7]
    density_c = shifted(density_pad, 0, 0, 0)
    flow_c = shifted(flow_pad, 0, 0, 0)
    magnet_c = shifted(magnet_pad, 0, 0, 0)
    press_c = shifted(press_pad, 0, 0, 0)
    momentum = density_pad[None] * flow_pad
    emf_pad = cross_of(flow_pad, magnet_pad)
    lorentz = cross_of(curl_of(magnet_pad), magnet_c)

    def carried(field):
        return flow_c[0] * radial_diff(field) + flow_c[1] * colat_diff(field) + flow_c[2] * lon_diff(field)

    div_mom = radial_diff(momentum[0]) + colat_diff(momentum[1]) + lon_diff(momentum[2])
    div_flow = radial_diff(flow_pad[0]) + colat_diff(flow_pad[1]) + lon_diff(flow_pad[2])
    press_grad = [radial_diff(press_pad), colat_diff(press_pad), lon_diff(press_pad)]
    new_density = density_c - dt_step * div_mom
    new_flow = jnp.stack([flow_c[comp] + dt_step * (-carried(flow_pad[comp]) + (lorentz[comp] - press_grad[comp]) / density_c + diffusivity * laplace(flow_pad[comp])) for comp in range(3)])
    new_magnet = magnet_c + dt_step * (curl_of(emf_pad) + diffusivity * laplace(magnet_pad))
    new_press = press_c + dt_step * (-carried(press_pad) - GAMMA * press_c * div_flow + diffusivity * laplace(press_pad))
    return new_density, new_flow, new_magnet, new_press


def donor_values(fields, send_row, send_col, send_weight, send_turn):
    tile_first_rows = jnp.arange(N_THETA, dtype=jnp.int32)[:, None, None] * CT
    tile_first_cols = jnp.arange(N_PHI, dtype=jnp.int32)[None, :, None] * CP
    row_index = (tile_first_rows + send_row).reshape(-1)
    col_index = (tile_first_cols + send_col).reshape(-1)
    weight_row = send_weight[:, :, 0, :].reshape(-1)
    weight_col = send_weight[:, :, 1, :].reshape(-1)

    def corner(step_t, step_p):
        return fields[:, :, row_index + step_t, col_index + step_p]

    blended = bilinear(corner(0, 0), corner(0, 1), corner(1, 0), corner(1, 1), weight_row, weight_col)
    return turn_frame(blended, send_turn.reshape(-1))


def advance_patch(fields, border, radius, constants):
    d_theta, d_phi, dt_step, diffusivity = constants
    radial_pad = jnp.pad(fields, ((0, 0), (1, 1), (0, 0), (0, 0)), mode="edge")
    padded = jnp.pad(radial_pad, ((0, 0), (0, 0), (1, 1), (1, 1)))
    upper_side = jnp.transpose(border[:NPH], (1, 2, 0))
    lower_side = jnp.transpose(border[NPH:2 * NPH], (1, 2, 0))
    left_side = jnp.transpose(border[2 * NPH:2 * NPH + NTH], (1, 2, 0))
    right_side = jnp.transpose(border[2 * NPH + NTH:], (1, 2, 0))
    padded = padded.at[:, 1:-1, 0, 1:-1].set(upper_side)
    padded = padded.at[:, 1:-1, -1, 1:-1].set(lower_side)
    padded = padded.at[:, 1:-1, 1:-1, 0].set(left_side)
    padded = padded.at[:, 1:-1, 1:-1, -1].set(right_side)

    def one_block(tile_number):
        first_row = tile_number * CT
        tile_block = lax.dynamic_slice_in_dim(padded, first_row, CT + 2, 2)
        rows_global = first_row + jnp.arange(CT, dtype=jnp.int32)
        sin_theta = jnp.sin(0.25 * math.pi + (rows_global.astype(jnp.float32) + 0.5) * d_theta)
        return advance(tile_block, radius, sin_theta, d_theta, d_phi, dt_step, diffusivity)

    blocks = lax.map(one_block, jnp.arange(N_THETA, dtype=jnp.int32))
    new_density = jnp.moveaxis(blocks[0], 0, -3).reshape(NR, NTH, NPH)
    new_flow = jnp.moveaxis(blocks[1], 0, -3).reshape(3, NR, NTH, NPH)
    new_magnet = jnp.moveaxis(blocks[2], 0, -3).reshape(3, NR, NTH, NPH)
    new_press = jnp.moveaxis(blocks[3], 0, -3).reshape(NR, NTH, NPH)
    return new_density, new_flow, new_magnet, new_press


def reference(density, velocity, magnetic, pressure, send_row, send_col, send_weight, send_turn, send_dest):
    fields = jnp.concatenate([density[:, None], velocity, magnetic, pressure[:, None]], axis=1)
    border_count = 2 * NPH + 2 * NTH
    constants = grid_constants(NTH, NPH)
    radius = R_BASE + (jnp.arange(NR, dtype=jnp.float32) + 0.5) * DR_STEP
    received = []
    for donor_patch in range(2):
        values = donor_values(fields[donor_patch], send_row[donor_patch], send_col[donor_patch], send_weight[donor_patch], send_turn[donor_patch])
        target = send_dest[donor_patch].reshape(-1)
        placed = jnp.zeros((border_count + 1, 8, NR), jnp.float32).at[target].add(jnp.transpose(values, (2, 0, 1)))
        received.append(placed[:border_count])
    results = [advance_patch(fields[which], received[1 - which], radius, constants) for which in range(2)]
    return (jnp.stack([results[0][0], results[1][0]]),
            jnp.stack([results[0][1], results[1][1]]),
            jnp.stack([results[0][2], results[1][2]]),
            jnp.stack([results[0][3], results[1][3]]))
```

```python
import functools
import math

import jax
import jax.numpy as jnp
from jax import lax
from jax.experimental import pallas as pl
from jax.experimental.pallas import tpu as pltpu
from jax.sharding import PartitionSpec as P

MESH = pl.DeviceIdType.MESH
F32 = jnp.float32
BF16 = jnp.bfloat16

GAMMA = 5.0 / 3.0
R_BASE = 0.6
DR_STEP = 0.65 / 64.0
COURANT = 0.4
DIFFUSE = 0.4

NR, CT, CP = 16, 16, 128
NZ, NF = 32, 16
NPH, NTH = CP * NF, CT * NZ
SEND = 96
CH = 8 * NR
HUBS = (0, NZ - 1, 8, 24)
SOURCES = 2 * NF + 2 * (NZ - 2)
SLOT_ROWS = 96 * 8


def grid_constants(total_theta, total_phi):
    d_theta = 0.5 * math.pi / total_theta
    d_phi = 1.5 * math.pi / total_phi
    r_low = R_BASE + 0.5 * DR_STEP
    inv_r = 1.0 / DR_STEP
    inv_t = 1.0 / (r_low * d_theta)
    inv_p = 1.0 / (r_low * math.sin(0.25 * math.pi) * d_phi)
    dt_step = COURANT / (inv_r + inv_t + inv_p)
    diffusivity = DIFFUSE / (dt_step * (inv_r * inv_r + inv_t * inv_t + inv_p * inv_p))
    return (d_theta, d_phi, dt_step, diffusivity)


def components(dens, vel, mag, pres):
    return [dens, vel.at[0], vel.at[1], vel.at[2], mag.at[0], mag.at[1], mag.at[2], pres]


def iota(shape, dim):
    return lax.broadcasted_iota(jnp.int32, shape, dim)


def pack_kernel(
    dens, vel, mag, pres, row_in, col_in, weight_in, turn_in, dest_in,
    first_row, last_row, left_col, right_col, donors, ints, floats,
):
    z = lax.axis_index("theta")
    f = lax.axis_index("phi")
    comps = components(dens, vel, mag, pres)
    for c in range(8):
        first_row[c * NR : (c + 1) * NR, :] = comps[c][:, 0, :]
        last_row[c * NR : (c + 1) * NR, :] = comps[c][:, CT - 1, :]
    lane = iota((CT, CP), 1)
    low = jnp.zeros((CT, CP), F32)
    high = jnp.zeros((CT, CP), F32)
    for c in range(8):
        for k in range(NR):
            ck = c * NR + k
            block = comps[c][k]
            low = jnp.where(lane == ck, pltpu.roll(block, ck, 1) if ck else block, low)
            shift = (ck + 1) % CP
            high = jnp.where(lane == ck, pltpu.roll(block, shift, 1) if shift else block, high)
    left_col[...] = low
    right_col[...] = high

    @pl.when((z == 0) | (z == NZ - 1) | (f == 0) | (f == NF - 1))
    def _():
        ints[...] = jnp.zeros_like(ints)
        floats[...] = jnp.zeros_like(floats)
        ints[0:1, 0:SEND] = row_in[...]
        ints[1:2, 0:SEND] = col_in[...]
        ints[2:3, 0:SEND] = jnp.where(dest_in[...] < 2 * (NPH + NTH), dest_in[...] + 1, 0)
        floats[0:2, 0:SEND] = weight_in[...]
        floats[2:3, 0:SEND] = turn_in[...]
        row, col, dest = ints[0:1, :], ints[1:2, :], ints[2:3, :]
        weight_row, weight_col, turn = floats[0:1, :], floats[1:2, :], floats[2:3, :]
        cell = iota((CP, CP), 0)
        col_mix = jnp.where(cell == col, 1.0 - weight_col, 0.0) + jnp.where(
            cell == col + 1, weight_col, 0.0
        )
        level = iota((CT, CP), 0)
        row_mix = jnp.where(level == row, 1.0 - weight_row, 0.0) + jnp.where(
            level == row + 1, weight_row, 0.0
        )
        value = jnp.zeros((CH, CP), F32)
        for i in range(CT):
            line = jnp.concatenate([comps[c][:, i, :] for c in range(8)], axis=0)
            mixed = jnp.dot(
                line, col_mix, preferred_element_type=F32, precision=lax.Precision.HIGHEST
            )
            value = value + row_mix[i : i + 1, :] * mixed
        cos_t, sin_t = jnp.cos(turn), jnp.sin(turn)
        part = [value[c * NR : (c + 1) * NR, :] for c in range(8)]
        turned = jnp.concatenate(
            [
                part[0],
                part[1],
                cos_t * part[2] + sin_t * part[3],
                cos_t * part[3] - sin_t * part[2],
                part[4],
                cos_t * part[5] + sin_t * part[6],
                cos_t * part[6] - sin_t * part[5],
                part[7],
            ],
            axis=0,
        )
        slots = turned.T
        for r in range(6):
            donors[pl.ds(r, 16, stride=8), :] = slots[16 * r : 16 * r + 16, :]
        where_z = jnp.where(z == 0, f, jnp.where(z == NZ - 1, NF + f, 0))
        where_f = jnp.where(f == 0, 2 * NF + z - 1, 2 * NF + NZ - 2 + z - 1)
        source = jnp.where((z == 0) | (z == NZ - 1), where_z, where_f)
        base = 8 * lax.rem(source, 16)
        slot = iota((16, CP), 1)
        group = iota((16, CP), 0)
        named = jnp.where(lax.rem(slot, 16) == group, dest.astype(F32), 0.0)
        slot_down = iota((CP, CP), 0)
        placed = jnp.where(iota((CP, CP), 1) == base + slot_down // 16, 1.0, 0.0)
        donors[pl.ds(6, 16, stride=8), :] = jnp.dot(
            named, placed, preferred_element_type=F32, precision=lax.Precision.HIGHEST
        )
        donors[pl.ds(7, 16, stride=8), :] = jnp.zeros((16, CP), F32)


def route_kernel(
    first_row, last_row, left_col, right_col, donors,
    out_top, out_bottom, out_left, out_right,
    top, bottom, left, right, slots, pieces, dense, inbox, total,
    halo_send, halo_recv, donor_send, donor_recv, dense_send, dense_recv, column_send,
):
    p = lax.axis_index("patch")
    z = lax.axis_index("theta")
    f = lax.axis_index("phi")
    on_row = (z == 0) | (z == NZ - 1)
    on_column = (f == 0) | (f == NF - 1)
    is_source = on_row | on_column
    column_hub = (z == HUBS[2]) | (z == HUBS[3])
    is_hub = on_row | column_hub
    half = z // 16
    hub_low = 16 * (z // 16)

    barrier = pltpu.get_barrier_semaphore()

    def greet(device):
        pl.semaphore_signal(barrier, inc=1, device_id=device, device_id_type=MESH)

    for has, device in (
        (z > 0, (p, z - 1, f)),
        (z < NZ - 1, (p, z + 1, f)),
        (f > 0, (p, z, f - 1)),
        (f < NF - 1, (p, z, f + 1)),
    ):
        pl.when(has)(functools.partial(greet, device))

    @pl.when(is_hub)
    def _():
        @pl.loop(0, NF)
        def _(j):
            greet((1 - p, 0, j))
            greet((1 - p, NZ - 1, j))

        @pl.loop(1, NZ - 1)
        def _(j):
            greet((1 - p, j, 0))
            greet((1 - p, j, NF - 1))

        @pl.loop(1, NF)
        def _(off):
            greet((p, z, lax.rem(f + off, NF)))

    @pl.when(on_column)
    def _():
        greet((p, HUBS[2] + 16 * half, z - 16 * half))

    @pl.when(is_hub)
    def _():
        slots[8 * SOURCES : SLOT_ROWS, :] = jnp.zeros((SLOT_ROWS - 8 * SOURCES, CP), F32)

    peers = (
        jnp.where(z > 0, 1, 0)
        + jnp.where(z < NZ - 1, 1, 0)
        + jnp.where(f > 0, 1, 0)
        + jnp.where(f < NF - 1, 1, 0)
        + jnp.where(is_hub, NF - 1, 0)
        + jnp.where(column_hub, 2, 0)
        + jnp.where(is_source, 4 * NF, 0)
    )
    pl.semaphore_wait(barrier, peers)

    def halo(which):
        src, dst, device = (
            (last_row, top, (p, z + 1, f)),
            (first_row, bottom, (p, z - 1, f)),
            (right_col, left, (p, z, f + 1)),
            (left_col, right, (p, z, f - 1)),
        )[which]
        return pltpu.make_async_remote_copy(
            src_ref=src,
            dst_ref=dst,
            send_sem=halo_send.at[which],
            recv_sem=halo_recv.at[which],
            device_id=device,
            device_id_type=MESH,
        )

    sends_to = (z < NZ - 1, z > 0, f < NF - 1, f > 0)
    hears_from = (z > 0, z < NZ - 1, f > 0, f < NF - 1)

    source = jnp.where(
        z == 0,
        f,
        jnp.where(z == NZ - 1, NF + f, jnp.where(f == 0, 2 * NF + z - 1, 2 * NF + NZ - 3 + z)),
    )

    def donor_copy(hub, plane, j):
        return pltpu.make_async_remote_copy(
            src_ref=donors.at[pl.ds(pl.multiple_of(8 * j, 8), 8)],
            dst_ref=slots.at[pl.ds(pl.multiple_of(8 * source, 8), 8)],
            send_sem=donor_send.at[hub],
            recv_sem=donor_recv,
            device_id=(1 - p, plane, j),
            device_id_type=MESH,
        )

    @pl.when(is_source)
    def _():
        @pl.loop(0, NF)
        def _(off):
            j = lax.rem(f + off, NF)
            for hub, plane in enumerate(HUBS):
                donor_copy(hub, plane, j).start()

    for which in range(4):

        @pl.when(sends_to[which])
        def _():
            halo(which).start()

    def whole_wait(ref, sem):
        return pltpu.make_async_copy(ref, ref, sem).wait()

    def split_slots():
        value = slots[...]
        high = value.astype(BF16)
        rest = value - high.astype(F32)
        mid = rest.astype(BF16)
        pieces[:, 0:CP] = high
        pieces[:, CP : 2 * CP] = mid
        pieces[:, 2 * CP :] = (rest - mid.astype(F32)).astype(BF16)
        ids = slots[pl.ds(6, 96, stride=8), :]
        return jnp.concatenate(
            [jnp.sum(ids[16 * g : 16 * g + 16, :], axis=0, keepdims=True) for g in range(6)],
            axis=1,
        )

    def place(ids, wanted):
        hits = jnp.where(ids == wanted.astype(F32), 1.0, 0.0).astype(BF16)
        out = jnp.dot(hits, pieces[...], preferred_element_type=F32)
        return out[:, 0:CP] + out[:, CP : 2 * CP] + out[:, 2 * CP :]

    point = iota((CP, 1), 0)

    def block_copy(rows, j):
        return pltpu.make_async_remote_copy(
            src_ref=dense.at[pl.ds(pl.multiple_of(rows * j, rows), rows)],
            dst_ref=inbox.at[pl.ds(pl.multiple_of(rows * f, rows), rows)],
            send_sem=dense_send,
            recv_sem=dense_recv,
            device_id=(p, z, j),
            device_id_type=MESH,
        )

    def gather_blocks(rows):
        whole_wait(inbox.at[pl.ds(0, rows * (NF - 1))], dense_recv)
        own = dense[pl.ds(pl.multiple_of(rows * f, rows), rows), :]

        def step(off, acc):
            j = lax.rem(f + off, NF)
            return acc + inbox[pl.ds(pl.multiple_of(rows * j, rows), rows), :]

        return lax.fori_loop(1, NF, step, own)

    @pl.when(on_row)
    def _():
        whole_wait(slots.at[pl.ds(0, 8 * SOURCES)], donor_recv)
        ids = split_slots()
        first = 1 + jnp.where(z == 0, 0, NPH)

        @pl.loop(1, NF + 1)
        def _(off):
            j = lax.rem(f + off, NF)
            dense[pl.ds(pl.multiple_of(CP * j, CP), CP), :] = place(ids, first + CP * j + point)

            @pl.when(off > 1)
            def _():
                block_copy(CP, lax.rem(f + off - 1, NF)).start()

        border = gather_blocks(CP).T

        @pl.when(z == 0)
        def _():
            top[...] = border

        @pl.when(z == NZ - 1)
        def _():
            bottom[...] = border

        whole_wait(dense.at[pl.ds(0, CP * (NF - 1))], dense_send)

    @pl.when(column_hub)
    def _():
        whole_wait(slots.at[pl.ds(0, 8 * SOURCES)], donor_recv)
        ids = split_slots()
        side = lax.rem(point, 32) // 16
        first = 1 + 2 * NPH + NTH * side + lax.rem(point, 16) + CT * (hub_low + point // 32)

        @pl.loop(0, 4)
        def _(quad):
            dense[pl.ds(pl.multiple_of(CP * quad, CP), CP), :] = place(ids, first + CT * 4 * quad)

        @pl.loop(1, NF)
        def _(off):
            block_copy(32, lax.rem(f + off, NF)).start()

        total[...] = gather_blocks(32)

        def forward(side_of, dst):
            return pltpu.make_async_remote_copy(
                src_ref=total.at[pl.ds(16 * side_of, 16)],
                dst_ref=dst,
                send_sem=column_send.at[side_of],
                recv_sem=halo_recv.at[2 + side_of],
                device_id=(p, hub_low + f, (NF - 1) * side_of),
                device_id_type=MESH,
            )

        copies = [forward(0, left), forward(1, right)]
        for copy in copies:
            copy.start()
        whole_wait(dense.at[pl.ds(0, 32 * (NF - 1))], dense_send)
        for copy in copies:
            copy.wait_send()

    for which, ref in enumerate((top, bottom)):

        @pl.when(hears_from[which])
        def _():
            whole_wait(ref, halo_recv.at[which])

    for which, ref in ((2, left), (3, right)):
        whole_wait(ref, halo_recv.at[which])

    out_top[...] = top[...]
    out_bottom[...] = bottom[...]
    out_left[...] = left[...]
    out_right[...] = right[...]

    for which in range(4):

        @pl.when(sends_to[which])
        def _():
            halo(which).wait_send()

    @pl.when(is_source)
    def _():
        for hub in range(4):
            whole_wait(donors, donor_send.at[hub])


def step_kernel(
    constants, dens, vel, mag, pres, top, bottom, left, right,
    new_dens, new_vel, new_mag, new_pres,
):
    d_theta, d_phi, dt, nu = constants
    z = lax.axis_index("theta")
    comps = components(dens, vel, mag, pres)
    row = iota((CT, CP), 0)
    lane = iota((CT, CP), 1)
    angle = 0.25 * math.pi + ((z * CT + row).astype(F32) + 0.5) * d_theta
    inv_sin = 1.0 / jnp.sin(angle)
    inv_sin_sq = inv_sin * inv_sin
    left_all, right_all = left[...], right[...]
    gr = 1.0 / DR_STEP

    for k in range(NR):
        radius = R_BASE + (k + 0.5) * DR_STEP
        gt = 1.0 / (radius * d_theta)
        gp = 1.0 / (radius * d_phi)
        hr, ht, hp = 0.5 * gr, 0.5 * gt, (0.5 * gp) * inv_sin
        lr, lt, lp = nu * gr * gr, nu * gt * gt, (nu * gp * gp) * inv_sin_sq
        C, U, D, N, S, W, E = ([], [], [], [], [], [], [])
        for c in range(8):
            ck = c * NR + k
            here = comps[c][k]
            C.append(here)
            U.append(comps[c][min(k + 1, NR - 1)])
            D.append(comps[c][max(k - 1, 0)])
            N.append(jnp.where(row == 0, top[ck : ck + 1, :], pltpu.roll(here, 1, 0)))
            S.append(jnp.where(row == CT - 1, bottom[ck : ck + 1, :], pltpu.roll(here, CT - 1, 0)))
            shift_w, shift_e = (CP - ck) % CP, (CP - 1 - ck) % CP
            edge_w = pltpu.roll(left_all, shift_w, 1) if shift_w else left_all
            edge_e = pltpu.roll(right_all, shift_e, 1) if shift_e else right_all
            W.append(jnp.where(lane == 0, edge_w, pltpu.roll(here, 1, 1)))
            E.append(jnp.where(lane == CP - 1, edge_e, pltpu.roll(here, CP - 1, 1)))

        def dr(c):
            return (U[c] - D[c]) * hr

        def dt_(c):
            return (S[c] - N[c]) * ht

        def dp(c):
            return (E[c] - W[c]) * hp

        def laplace(c):
            twice = 2.0 * C[c]
            return (
                (U[c] + D[c] - twice) * lr
                + (S[c] + N[c] - twice) * lt
                + (E[c] + W[c] - twice) * lp
            )

        def emf(side, comp):
            a, b = (((2, 6), (3, 5)), ((3, 4), (1, 6)), ((1, 5), (2, 4)))[comp]
            return side[a[0]] * side[a[1]] - side[b[0]] * side[b[1]]

        rho, p = C[0], C[7]
        v = C[1:4]
        b = C[4:7]
        grad_v = [(dr(c), dt_(c), dp(c)) for c in (1, 2, 3)]
        grad_p = (dr(7), dt_(7), dp(7))
        div_mom = (
            (U[0] * U[1] - D[0] * D[1]) * hr
            + (S[0] * S[2] - N[0] * N[2]) * ht
            + (E[0] * E[3] - W[0] * W[3]) * hp
        )
        new_dens[k] = rho - dt * div_mom
        j_r = dt_(6) - dp(5)
        j_t = dp(4) - dr(6)
        j_p = dr(5) - dt_(4)
        force = (j_t * b[2] - j_p * b[1], j_p * b[0] - j_r * b[2], j_r * b[1] - j_t * b[0])
        inv_rho = 1.0 / rho

        def carried(grad):
            return v[0] * grad[0] + v[1] * grad[1] + v[2] * grad[2]

        for c in range(3):
            new_vel[c, k] = v[c] + dt * (
                (force[c] - grad_p[c]) * inv_rho - carried(grad_v[c]) + laplace(1 + c)
            )
        div_v = grad_v[0][0] + grad_v[1][1] + grad_v[2][2]
        new_pres[k] = p + dt * (laplace(7) - carried(grad_p) - GAMMA * p * div_v)
        dt_ep = (emf(S, 2) - emf(N, 2)) * ht
        dp_et = (emf(E, 1) - emf(W, 1)) * hp
        dp_er = (emf(E, 0) - emf(W, 0)) * hp
        dr_ep = (emf(U, 2) - emf(D, 2)) * hr
        dr_et = (emf(U, 1) - emf(D, 1)) * hr
        dt_er = (emf(S, 0) - emf(N, 0)) * ht
        new_mag[0, k] = b[0] + dt * (dt_ep - dp_et + laplace(4))
        new_mag[1, k] = b[1] + dt * (dp_er - dr_ep + laplace(5))
        new_mag[2, k] = b[2] + dt * (dr_et - dt_er + laplace(6))


VMEM = pl.BlockSpec(memory_space=pltpu.VMEM)


def shape(*dims):
    return jax.ShapeDtypeStruct(dims, F32)


def body(
    density, velocity, magnetic, pressure, send_row, send_col, send_weight, send_turn, send_dest
):
    fields = (density[0], velocity[0], magnetic[0], pressure[0])
    packed = pl.pallas_call(
        pack_kernel,
        out_shape=(shape(CH, CP), shape(CH, CP), shape(CT, CP), shape(CT, CP), shape(CP, CP)),
        in_specs=[VMEM] * 9,
        out_specs=(VMEM,) * 5,
        scratch_shapes=[pltpu.VMEM((8, CP), jnp.int32), pltpu.VMEM((8, CP), F32)],
        name="pack",
    )(
        *fields,
        send_row.reshape(1, SEND),
        send_col.reshape(1, SEND),
        send_weight.reshape(2, SEND),
        send_turn.reshape(1, SEND),
        send_dest.reshape(1, SEND),
    )
    halos = pl.pallas_call(
        route_kernel,
        out_shape=(shape(CH, CP), shape(CH, CP), shape(CT, CP), shape(CT, CP)),
        in_specs=[VMEM] * 5,
        out_specs=(VMEM,) * 4,
        scratch_shapes=[
            pltpu.VMEM((CH, CP), F32),
            pltpu.VMEM((CH, CP), F32),
            pltpu.VMEM((CT, CP), F32),
            pltpu.VMEM((CT, CP), F32),
            pltpu.VMEM((SLOT_ROWS, CP), F32),
            pltpu.VMEM((SLOT_ROWS, 3 * CP), BF16),
            pltpu.VMEM((NF * CP, CP), F32),
            pltpu.VMEM((NF * CP, CP), F32),
            pltpu.VMEM((32, CP), F32),
            pltpu.SemaphoreType.DMA((4,)),
            pltpu.SemaphoreType.DMA((4,)),
            pltpu.SemaphoreType.DMA((4,)),
            pltpu.SemaphoreType.DMA,
            pltpu.SemaphoreType.DMA,
            pltpu.SemaphoreType.DMA,
            pltpu.SemaphoreType.DMA((2,)),
        ],
        compiler_params=pltpu.CompilerParams(collective_id=0, has_side_effects=True),
        name="route",
    )(*packed)
    new_density, new_flow, new_magnet, new_press = pl.pallas_call(
        functools.partial(step_kernel, grid_constants(NTH, NPH)),
        out_shape=(shape(NR, CT, CP), shape(3, NR, CT, CP), shape(3, NR, CT, CP), shape(NR, CT, CP)),
        in_specs=[VMEM] * 8,
        out_specs=(VMEM,) * 4,
        name="step",
    )(*fields, *halos)
    return (new_density[None], new_flow[None], new_magnet[None], new_press[None])


def solution(mesh):
    return jax.shard_map(
        body,
        mesh=mesh,
        in_specs=(
            P("patch", None, "theta", "phi"),
            P("patch", None, None, "theta", "phi"),
            P("patch", None, None, "theta", "phi"),
            P("patch", None, "theta", "phi"),
            P("patch", "theta", "phi", None),
            P("patch", "theta", "phi", None),
            P("patch", "theta", "phi", None, None),
            P("patch", "theta", "phi", None),
            P("patch", "theta", "phi", None),
        ),
        out_specs=(
            P("patch", None, "theta", "phi"),
            P("patch", None, None, "theta", "phi"),
            P("patch", None, None, "theta", "phi"),
            P("patch", None, "theta", "phi"),
        ),
        check_vma=False,
    )
```

```python
import functools
import math

import jax
import jax.numpy as jnp
from jax import lax
from jax.experimental import pallas as pl
from jax.experimental.pallas import tpu as pltpu
from jax.sharding import PartitionSpec as P

MESH = pl.DeviceIdType.MESH
F32 = jnp.float32
BF16 = jnp.bfloat16

GAMMA = 5.0 / 3.0
R_BASE = 0.6
DR_STEP = 0.65 / 64.0
COURANT = 0.4
DIFFUSE = 0.4

NR, CT, CP = 16, 16, 128
NZ, NF = 32, 16
NPH, NTH = CP * NF, CT * NZ
SEND = 96
CH = 8 * NR
HUBS = (0, NZ - 1, 8, 24)
SOURCES = 2 * NF + 2 * (NZ - 2)
SLOT_ROWS = 96 * 8


def grid_constants(total_theta, total_phi):
    d_theta = 0.5 * math.pi / total_theta
    d_phi = 1.5 * math.pi / total_phi
    r_low = R_BASE + 0.5 * DR_STEP
    inv_r = 1.0 / DR_STEP
    inv_t = 1.0 / (r_low * d_theta)
    inv_p = 1.0 / (r_low * math.sin(0.25 * math.pi) * d_phi)
    dt_step = COURANT / (inv_r + inv_t + inv_p)
    diffusivity = DIFFUSE / (dt_step * (inv_r * inv_r + inv_t * inv_t + inv_p * inv_p))
    return (d_theta, d_phi, dt_step, diffusivity)


def components(dens, vel, mag, pres):
    return [dens, vel.at[0], vel.at[1], vel.at[2], mag.at[0], mag.at[1], mag.at[2], pres]


def iota(shape, dim):
    return lax.broadcasted_iota(jnp.int32, shape, dim)


def pack(
    dens, vel, mag, pres, row_in, col_in, weight_in, turn_in, dest_in,
    first_row, last_row, left_col, right_col, donors, ints, floats,
):
    z = lax.axis_index("theta")
    f = lax.axis_index("phi")
    comps = components(dens, vel, mag, pres)
    for c in range(8):
        first_row[c * NR : (c + 1) * NR, :] = comps[c][:, 0, :]
        last_row[c * NR : (c + 1) * NR, :] = comps[c][:, CT - 1, :]
    lane = iota((CT, CP), 1)
    low = jnp.zeros((CT, CP), F32)
    high = jnp.zeros((CT, CP), F32)
    for c in range(8):
        for k in range(NR):
            ck = c * NR + k
            block = comps[c][k]
            low = jnp.where(lane == ck, pltpu.roll(block, ck, 1) if ck else block, low)
            shift = (ck + 1) % CP
            high = jnp.where(lane == ck, pltpu.roll(block, shift, 1) if shift else block, high)
    left_col[...] = low
    right_col[...] = high

    @pl.when((z == 0) | (z == NZ - 1) | (f == 0) | (f == NF - 1))
    def _():
        ints[...] = jnp.zeros_like(ints)
        floats[...] = jnp.zeros_like(floats)
        ints[0:1, 0:SEND] = row_in[...]
        ints[1:2, 0:SEND] = col_in[...]
        ints[2:3, 0:SEND] = jnp.where(dest_in[...] < 2 * (NPH + NTH), dest_in[...] + 1, 0)
        floats[0:2, 0:SEND] = weight_in[...]
        floats[2:3, 0:SEND] = turn_in[...]
        row, col, dest = ints[0:1, :], ints[1:2, :], ints[2:3, :]
        weight_row, weight_col, turn = floats[0:1, :], floats[1:2, :], floats[2:3, :]
        cell = iota((CP, CP), 0)
        col_mix = jnp.where(cell == col, 1.0 - weight_col, 0.0) + jnp.where(
            cell == col + 1, weight_col, 0.0
        )
        level = iota((CT, CP), 0)
        row_mix = jnp.where(level == row, 1.0 - weight_row, 0.0) + jnp.where(
            level == row + 1, weight_row, 0.0
        )
        value = jnp.zeros((CH, CP), F32)
        for i in range(CT):
            line = jnp.concatenate([comps[c][:, i, :] for c in range(8)], axis=0)
            mixed = jnp.dot(
                line, col_mix, preferred_element_type=F32, precision=lax.Precision.HIGHEST
            )
            value = value + row_mix[i : i + 1, :] * mixed
        cos_t, sin_t = jnp.cos(turn), jnp.sin(turn)
        part = [value[c * NR : (c + 1) * NR, :] for c in range(8)]
        turned = jnp.concatenate(
            [
                part[0],
                part[1],
                cos_t * part[2] + sin_t * part[3],
                cos_t * part[3] - sin_t * part[2],
                part[4],
                cos_t * part[5] + sin_t * part[6],
                cos_t * part[6] - sin_t * part[5],
                part[7],
            ],
            axis=0,
        )
        slots = turned.T
        for r in range(6):
            donors[pl.ds(r, 16, stride=8), :] = slots[16 * r : 16 * r + 16, :]
        where_z = jnp.where(z == 0, f, jnp.where(z == NZ - 1, NF + f, 0))
        where_f = 2 * NF + 2 * (z - 1) + jnp.where(f == 0, 0, 1)
        source = jnp.where((z == 0) | (z == NZ - 1), where_z, where_f)
        base = 8 * lax.rem(source, 16)
        slot = iota((16, CP), 1)
        group = iota((16, CP), 0)
        named = jnp.where(lax.rem(slot, 16) == group, dest.astype(F32), 0.0)
        slot_down = iota((CP, CP), 0)
        placed = jnp.where(iota((CP, CP), 1) == base + slot_down // 16, 1.0, 0.0)
        donors[pl.ds(6, 16, stride=8), :] = jnp.dot(
            named, placed, preferred_element_type=F32, precision=lax.Precision.HIGHEST
        )
        donors[pl.ds(7, 16, stride=8), :] = jnp.zeros((16, CP), F32)


def route_kernel(
    dens, vel, mag, pres, row_in, col_in, weight_in, turn_in, dest_in,
    out_top, out_bottom, out_left, out_right,
    first_row, last_row, left_col, right_col, donors, ints, floats,
    top, bottom, left, right, slots, pieces, dense, inbox, total,
    halo_send, halo_recv, donor_send, donor_recv, relay_send, relay_recv,
    dense_send, dense_recv, column_send,
):
    p = lax.axis_index("patch")
    z = lax.axis_index("theta")
    f = lax.axis_index("phi")
    on_row = (z == 0) | (z == NZ - 1)
    on_column = (f == 0) | (f == NF - 1)
    is_source = on_row | on_column
    column_hub = (z == HUBS[2]) | (z == HUBS[3])
    is_hub = on_row | column_hub
    half = z // 16
    hub_low = 16 * (z // 16)

    barrier = pltpu.get_barrier_semaphore()

    def greet(device):
        pl.semaphore_signal(barrier, inc=1, device_id=device, device_id_type=MESH)

    @pl.when(is_hub)
    def _():
        @pl.loop(1, NZ)
        def _(off):
            greet((p, lax.rem(z + off, NZ), f))

        @pl.loop(1, NF)
        def _(off):
            greet((p, z, lax.rem(f + off, NF)))

    @pl.when(on_row)
    def _():
        @pl.loop(0, NF)
        def _(j):
            greet((1 - p, z, j))

    @pl.when(jnp.logical_not(on_row))
    def _():
        greet((1 - p, z, 0))
        greet((1 - p, z, NF - 1))

    @pl.when(on_column)
    def _():
        greet((p, HUBS[2] + 16 * half, z - 16 * half))

    for has, device in (
        (z > 0, (p, z - 1, f)),
        (z < NZ - 1, (p, z + 1, f)),
        (f > 0, (p, z, f - 1)),
        (f < NF - 1, (p, z, f + 1)),
    ):
        pl.when(has)(functools.partial(greet, device))

    pack(
        dens, vel, mag, pres, row_in, col_in, weight_in, turn_in, dest_in,
        first_row, last_row, left_col, right_col, donors, ints, floats,
    )

    @pl.when(is_hub)
    def _():
        slots[8 * SOURCES : SLOT_ROWS, :] = jnp.zeros((SLOT_ROWS - 8 * SOURCES, CP), F32)

    peers = (
        jnp.where(z > 0, 1, 0)
        + jnp.where(z < NZ - 1, 1, 0)
        + jnp.where(f > 0, 1, 0)
        + jnp.where(f < NF - 1, 1, 0)
        + jnp.where(is_hub, NF - 1 + 3, 4)
        + jnp.where(column_hub, 2, 0)
        + jnp.where(is_source, NF, 0)
    )
    pl.semaphore_wait(barrier, peers)

    def halo(which):
        src, dst, device = (
            (last_row, top, (p, z + 1, f)),
            (first_row, bottom, (p, z - 1, f)),
            (right_col, left, (p, z, f + 1)),
            (left_col, right, (p, z, f - 1)),
        )[which]
        return pltpu.make_async_remote_copy(
            src_ref=src,
            dst_ref=dst,
            send_sem=halo_send.at[which],
            recv_sem=halo_recv.at[which],
            device_id=device,
            device_id_type=MESH,
        )

    sends_to = (z < NZ - 1, z > 0, f < NF - 1, f > 0)
    hears_from = (z > 0, z < NZ - 1, f > 0, f < NF - 1)

    plane_low = jnp.where(z == 0, 0, jnp.where(z == NZ - 1, NF, 2 * NF + 2 * (z - 1)))
    source = plane_low + jnp.where(on_row, f, jnp.where(f == 0, 0, 1))

    @pl.when(is_source)
    def _():
        @pl.loop(0, NF)
        def _(off):
            j = lax.rem(f + off, NF)
            pltpu.make_async_remote_copy(
                src_ref=donors.at[pl.ds(pl.multiple_of(8 * j, 8), 8)],
                dst_ref=slots.at[pl.ds(pl.multiple_of(8 * source, 8), 8)],
                send_sem=donor_send,
                recv_sem=donor_recv,
                device_id=(1 - p, z, j),
                device_id_type=MESH,
            ).start()

    for which in range(4):

        @pl.when(sends_to[which])
        def _():
            halo(which).start()

    def whole_wait(ref, sem):
        return pltpu.make_async_copy(ref, ref, sem).wait()

    def relay(tiles, hub):
        rows = slots.at[pl.ds(pl.multiple_of(8 * plane_low, 8), 8 * tiles)]
        return pltpu.make_async_remote_copy(
            src_ref=rows,
            dst_ref=rows,
            send_sem=relay_send.at[hub],
            recv_sem=relay_recv,
            device_id=(p, HUBS[hub], f),
            device_id_type=MESH,
        )

    for here, tiles in ((on_row, NF), (jnp.logical_not(on_row), 2)):

        @pl.when(here)
        def _():
            whole_wait(slots.at[pl.ds(0, 8 * tiles)], donor_recv)
            for hub in range(4):

                @pl.when(z != HUBS[hub])
                def _():
                    relay(tiles, hub).start()

    def split_slots():
        value = slots[...]
        high = value.astype(BF16)
        rest = value - high.astype(F32)
        mid = rest.astype(BF16)
        pieces[:, 0:CP] = high
        pieces[:, CP : 2 * CP] = mid
        pieces[:, 2 * CP :] = (rest - mid.astype(F32)).astype(BF16)
        ids = slots[pl.ds(6, 96, stride=8), :]
        return jnp.concatenate(
            [jnp.sum(ids[16 * g : 16 * g + 16, :], axis=0, keepdims=True) for g in range(6)],
            axis=1,
        )

    def place(ids, wanted):
        hits = jnp.where(ids == wanted.astype(F32), 1.0, 0.0).astype(BF16)
        out = jnp.dot(hits, pieces[...], preferred_element_type=F32)
        return out[:, 0:CP] + out[:, CP : 2 * CP] + out[:, 2 * CP :]

    point = iota((CP, 1), 0)

    def block_copy(rows, j):
        return pltpu.make_async_remote_copy(
            src_ref=dense.at[pl.ds(pl.multiple_of(rows * j, rows), rows)],
            dst_ref=inbox.at[pl.ds(pl.multiple_of(rows * f, rows), rows)],
            send_sem=dense_send,
            recv_sem=dense_recv,
            device_id=(p, z, j),
            device_id_type=MESH,
        )

    def gather_blocks(rows):
        whole_wait(inbox.at[pl.ds(0, rows * (NF - 1))], dense_recv)
        own = dense[pl.ds(pl.multiple_of(rows * f, rows), rows), :]

        def step(off, acc):
            j = lax.rem(f + off, NF)
            return acc + inbox[pl.ds(pl.multiple_of(rows * j, rows), rows), :]

        return lax.fori_loop(1, NF, step, own)

    @pl.when(on_row)
    def _():
        whole_wait(slots.at[pl.ds(0, 8 * (SOURCES - NF))], relay_recv)
        ids = split_slots()
        first = 1 + jnp.where(z == 0, 0, NPH)

        @pl.loop(1, NF + 1)
        def _(off):
            j = lax.rem(f + off, NF)
            dense[pl.ds(pl.multiple_of(CP * j, CP), CP), :] = place(ids, first + CP * j + point)

            @pl.when(off > 1)
            def _():
                block_copy(CP, lax.rem(f + off - 1, NF)).start()

        border = gather_blocks(CP).T

        @pl.when(z == 0)
        def _():
            top[...] = border

        @pl.when(z == NZ - 1)
        def _():
            bottom[...] = border

        whole_wait(dense.at[pl.ds(0, CP * (NF - 1))], dense_send)

    @pl.when(column_hub)
    def _():
        whole_wait(slots.at[pl.ds(0, 8 * (SOURCES - 2))], relay_recv)
        ids = split_slots()
        side = lax.rem(point, 32) // 16
        first = 1 + 2 * NPH + NTH * side + lax.rem(point, 16) + CT * (hub_low + point // 32)

        @pl.loop(0, 4)
        def _(quad):
            dense[pl.ds(pl.multiple_of(CP * quad, CP), CP), :] = place(ids, first + CT * 4 * quad)

        @pl.loop(1, NF)
        def _(off):
            block_copy(32, lax.rem(f + off, NF)).start()

        total[...] = gather_blocks(32)

        def forward(side_of, dst):
            return pltpu.make_async_remote_copy(
                src_ref=total.at[pl.ds(16 * side_of, 16)],
                dst_ref=dst,
                send_sem=column_send.at[side_of],
                recv_sem=halo_recv.at[2 + side_of],
                device_id=(p, hub_low + f, (NF - 1) * side_of),
                device_id_type=MESH,
            )

        copies = [forward(0, left), forward(1, right)]
        for copy in copies:
            copy.start()
        whole_wait(dense.at[pl.ds(0, 32 * (NF - 1))], dense_send)
        for copy in copies:
            copy.wait_send()

    for which, ref in enumerate((top, bottom)):

        @pl.when(hears_from[which])
        def _():
            whole_wait(ref, halo_recv.at[which])

    for which, ref in ((2, left), (3, right)):
        whole_wait(ref, halo_recv.at[which])

    out_top[...] = top[...]
    out_bottom[...] = bottom[...]
    out_left[...] = left[...]
    out_right[...] = right[...]

    for which in range(4):

        @pl.when(sends_to[which])
        def _():
            halo(which).wait_send()

    @pl.when(is_source)
    def _():
        whole_wait(donors, donor_send)

    for here, tiles in ((on_row, NF), (jnp.logical_not(on_row), 2)):
        for hub in range(4):

            @pl.when(here & (z != HUBS[hub]))
            def _():
                relay(tiles, hub).wait_send()


def step_kernel(
    constants, dens, vel, mag, pres, top, bottom, left, right,
    new_dens, new_vel, new_mag, new_pres,
):
    d_theta, d_phi, dt, nu = constants
    z = lax.axis_index("theta")
    comps = components(dens, vel, mag, pres)
    row = iota((CT, CP), 0)
    lane = iota((CT, CP), 1)
    angle = 0.25 * math.pi + ((z * CT + row).astype(F32) + 0.5) * d_theta
    inv_sin = 1.0 / jnp.sin(angle)
    inv_sin_sq = inv_sin * inv_sin
    left_all, right_all = left[...], right[...]
    gr = 1.0 / DR_STEP

    for k in range(NR):
        radius = R_BASE + (k + 0.5) * DR_STEP
        gt = 1.0 / (radius * d_theta)
        gp = 1.0 / (radius * d_phi)
        hr, ht, hp = 0.5 * gr, 0.5 * gt, (0.5 * gp) * inv_sin
        lr, lt, lp = nu * gr * gr, nu * gt * gt, (nu * gp * gp) * inv_sin_sq
        C, U, D, N, S, W, E = ([], [], [], [], [], [], [])
        for c in range(8):
            ck = c * NR + k
            here = comps[c][k]
            C.append(here)
            U.append(comps[c][min(k + 1, NR - 1)])
            D.append(comps[c][max(k - 1, 0)])
            N.append(jnp.where(row == 0, top[ck : ck + 1, :], pltpu.roll(here, 1, 0)))
            S.append(jnp.where(row == CT - 1, bottom[ck : ck + 1, :], pltpu.roll(here, CT - 1, 0)))
            shift_w, shift_e = (CP - ck) % CP, (CP - 1 - ck) % CP
            edge_w = pltpu.roll(left_all, shift_w, 1) if shift_w else left_all
            edge_e = pltpu.roll(right_all, shift_e, 1) if shift_e else right_all
            W.append(jnp.where(lane == 0, edge_w, pltpu.roll(here, 1, 1)))
            E.append(jnp.where(lane == CP - 1, edge_e, pltpu.roll(here, CP - 1, 1)))

        def dr(c):
            return (U[c] - D[c]) * hr

        def dt_(c):
            return (S[c] - N[c]) * ht

        def dp(c):
            return (E[c] - W[c]) * hp

        def laplace(c):
            twice = 2.0 * C[c]
            return (
                (U[c] + D[c] - twice) * lr
                + (S[c] + N[c] - twice) * lt
                + (E[c] + W[c] - twice) * lp
            )

        def emf(side, comp):
            a, b = (((2, 6), (3, 5)), ((3, 4), (1, 6)), ((1, 5), (2, 4)))[comp]
            return side[a[0]] * side[a[1]] - side[b[0]] * side[b[1]]

        rho, p = C[0], C[7]
        v = C[1:4]
        b = C[4:7]
        grad_v = [(dr(c), dt_(c), dp(c)) for c in (1, 2, 3)]
        grad_p = (dr(7), dt_(7), dp(7))
        div_mom = (
            (U[0] * U[1] - D[0] * D[1]) * hr
            + (S[0] * S[2] - N[0] * N[2]) * ht
            + (E[0] * E[3] - W[0] * W[3]) * hp
        )
        new_dens[k] = rho - dt * div_mom
        j_r = dt_(6) - dp(5)
        j_t = dp(4) - dr(6)
        j_p = dr(5) - dt_(4)
        force = (j_t * b[2] - j_p * b[1], j_p * b[0] - j_r * b[2], j_r * b[1] - j_t * b[0])
        inv_rho = 1.0 / rho

        def carried(grad):
            return v[0] * grad[0] + v[1] * grad[1] + v[2] * grad[2]

        for c in range(3):
            new_vel[c, k] = v[c] + dt * (
                (force[c] - grad_p[c]) * inv_rho - carried(grad_v[c]) + laplace(1 + c)
            )
        div_v = grad_v[0][0] + grad_v[1][1] + grad_v[2][2]
        new_pres[k] = p + dt * (laplace(7) - carried(grad_p) - GAMMA * p * div_v)
        dt_ep = (emf(S, 2) - emf(N, 2)) * ht
        dp_et = (emf(E, 1) - emf(W, 1)) * hp
        dp_er = (emf(E, 0) - emf(W, 0)) * hp
        dr_ep = (emf(U, 2) - emf(D, 2)) * hr
        dr_et = (emf(U, 1) - emf(D, 1)) * hr
        dt_er = (emf(S, 0) - emf(N, 0)) * ht
        new_mag[0, k] = b[0] + dt * (dt_ep - dp_et + laplace(4))
        new_mag[1, k] = b[1] + dt * (dp_er - dr_ep + laplace(5))
        new_mag[2, k] = b[2] + dt * (dr_et - dt_er + laplace(6))


VMEM = pl.BlockSpec(memory_space=pltpu.VMEM)


def shape(*dims):
    return jax.ShapeDtypeStruct(dims, F32)


def body(
    density, velocity, magnetic, pressure, send_row, send_col, send_weight, send_turn, send_dest
):
    fields = (density[0], velocity[0], magnetic[0], pressure[0])
    halos = pl.pallas_call(
        route_kernel,
        out_shape=(shape(CH, CP), shape(CH, CP), shape(CT, CP), shape(CT, CP)),
        in_specs=[VMEM] * 9,
        out_specs=(VMEM,) * 4,
        scratch_shapes=[
            pltpu.VMEM((CH, CP), F32),
            pltpu.VMEM((CH, CP), F32),
            pltpu.VMEM((CT, CP), F32),
            pltpu.VMEM((CT, CP), F32),
            pltpu.VMEM((CP, CP), F32),
            pltpu.VMEM((8, CP), jnp.int32),
            pltpu.VMEM((8, CP), F32),
            pltpu.VMEM((CH, CP), F32),
            pltpu.VMEM((CH, CP), F32),
            pltpu.VMEM((CT, CP), F32),
            pltpu.VMEM((CT, CP), F32),
            pltpu.VMEM((SLOT_ROWS, CP), F32),
            pltpu.VMEM((SLOT_ROWS, 3 * CP), BF16),
            pltpu.VMEM((NF * CP, CP), F32),
            pltpu.VMEM((NF * CP, CP), F32),
            pltpu.VMEM((32, CP), F32),
            pltpu.SemaphoreType.DMA((4,)),
            pltpu.SemaphoreType.DMA((4,)),
            pltpu.SemaphoreType.DMA,
            pltpu.SemaphoreType.DMA,
            pltpu.SemaphoreType.DMA((4,)),
            pltpu.SemaphoreType.DMA,
            pltpu.SemaphoreType.DMA,
            pltpu.SemaphoreType.DMA,
            pltpu.SemaphoreType.DMA((2,)),
        ],
        compiler_params=pltpu.CompilerParams(collective_id=0, has_side_effects=True),
        name="route",
    )(
        *fields,
        send_row.reshape(1, SEND),
        send_col.reshape(1, SEND),
        send_weight.reshape(2, SEND),
        send_turn.reshape(1, SEND),
        send_dest.reshape(1, SEND),
    )
    new_density, new_flow, new_magnet, new_press = pl.pallas_call(
        functools.partial(step_kernel, grid_constants(NTH, NPH)),
        out_shape=(shape(NR, CT, CP), shape(3, NR, CT, CP), shape(3, NR, CT, CP), shape(NR, CT, CP)),
        in_specs=[VMEM] * 8,
        out_specs=(VMEM,) * 4,
        name="step",
    )(*fields, *halos)
    return (new_density[None], new_flow[None], new_magnet[None], new_press[None])


def solution(mesh):
    return jax.shard_map(
        body,
        mesh=mesh,
        in_specs=(
            P("patch", None, "theta", "phi"),
            P("patch", None, None, "theta", "phi"),
            P("patch", None, None, "theta", "phi"),
            P("patch", None, "theta", "phi"),
            P("patch", "theta", "phi", None),
            P("patch", "theta", "phi", None),
            P("patch", "theta", "phi", None, None),
            P("patch", "theta", "phi", None),
            P("patch", "theta", "phi", None),
        ),
        out_specs=(
            P("patch", None, "theta", "phi"),
            P("patch", None, None, "theta", "phi"),
            P("patch", None, None, "theta", "phi"),
            P("patch", None, "theta", "phi"),
        ),
        check_vma=False,
    )
```

```python
import functools
import math

import jax
import jax.numpy as jnp
from jax import lax
from jax.experimental import pallas as pl
from jax.experimental.pallas import tpu as pltpu
from jax.sharding import PartitionSpec as P

MESH = pl.DeviceIdType.MESH
F32 = jnp.float32
BF16 = jnp.bfloat16

GAMMA = 5.0 / 3.0
R_BASE = 0.6
DR_STEP = 0.65 / 64.0
COURANT = 0.4
DIFFUSE = 0.4

NR, CT, CP = 16, 16, 128
NZ, NF = 32, 16
NPH, NTH = CP * NF, CT * NZ
SEND = 96
CH = 8 * NR
HUBS = (0, 1, 2, 20)
TOP_ROWS = (80, 48)
STEPS = (
    (2, 2), (2, 1), (1, 2), (2, 3), (3, 2), (1, 1), (3, 3), (1, 3), (3, 1),
    (2, 0), (0, 2), (1, 0), (0, 1), (3, 0), (0, 3),
)
SOURCES = 2 * NF + 2 * (NZ - 2)
SLOT_ROWS = 96 * 8


def grid_constants(total_theta, total_phi):
    d_theta = 0.5 * math.pi / total_theta
    d_phi = 1.5 * math.pi / total_phi
    r_low = R_BASE + 0.5 * DR_STEP
    inv_r = 1.0 / DR_STEP
    inv_t = 1.0 / (r_low * d_theta)
    inv_p = 1.0 / (r_low * math.sin(0.25 * math.pi) * d_phi)
    dt_step = COURANT / (inv_r + inv_t + inv_p)
    diffusivity = DIFFUSE / (dt_step * (inv_r * inv_r + inv_t * inv_t + inv_p * inv_p))
    return (d_theta, d_phi, dt_step, diffusivity)


def components(dens, vel, mag, pres):
    return [dens, vel.at[0], vel.at[1], vel.at[2], mag.at[0], mag.at[1], mag.at[2], pres]


def iota(shape, dim):
    return lax.broadcasted_iota(jnp.int32, shape, dim)


def pack(comps, first_row, last_row, left_col, right_col):
    for c in range(8):
        first_row[c * NR : (c + 1) * NR, :] = comps[c][:, 0, :]
        last_row[c * NR : (c + 1) * NR, :] = comps[c][:, CT - 1, :]
    lane = iota((CT, CP), 1)
    low = jnp.zeros((CT, CP), F32)
    high = jnp.zeros((CT, CP), F32)
    for c in range(8):
        for k in range(NR):
            ck = c * NR + k
            block = comps[c][k]
            low = jnp.where(lane == ck, pltpu.roll(block, ck, 1) if ck else block, low)
            shift = (ck + 1) % CP
            high = jnp.where(lane == ck, pltpu.roll(block, shift, 1) if shift else block, high)
    left_col[...] = low
    right_col[...] = high


def find_donors(source, comps, row_in, col_in, weight_in, turn_in, dest_in, donors, ints, floats):
    ints[...] = jnp.zeros_like(ints)
    floats[...] = jnp.zeros_like(floats)
    ints[0:1, 0:SEND] = row_in[...]
    ints[1:2, 0:SEND] = col_in[...]
    ints[2:3, 0:SEND] = jnp.where(dest_in[...] < 2 * (NPH + NTH), dest_in[...] + 1, 0)
    floats[0:2, 0:SEND] = weight_in[...]
    floats[2:3, 0:SEND] = turn_in[...]
    row, col, dest = ints[0:1, :], ints[1:2, :], ints[2:3, :]
    weight_row, weight_col, turn = floats[0:1, :], floats[1:2, :], floats[2:3, :]
    cell = iota((CP, CP), 0)
    col_mix = jnp.where(cell == col, 1.0 - weight_col, 0.0) + jnp.where(
        cell == col + 1, weight_col, 0.0
    )
    level = iota((CT, CP), 0)
    row_mix = jnp.where(level == row, 1.0 - weight_row, 0.0) + jnp.where(
        level == row + 1, weight_row, 0.0
    )
    value = jnp.zeros((CH, CP), F32)
    for i in range(CT):
        line = jnp.concatenate([comps[c][:, i, :] for c in range(8)], axis=0)
        mixed = jnp.dot(
            line, col_mix, preferred_element_type=F32, precision=lax.Precision.HIGHEST
        )
        value = value + row_mix[i : i + 1, :] * mixed
    cos_t, sin_t = jnp.cos(turn), jnp.sin(turn)
    part = [value[c * NR : (c + 1) * NR, :] for c in range(8)]
    turned = jnp.concatenate(
        [
            part[0],
            part[1],
            cos_t * part[2] + sin_t * part[3],
            cos_t * part[3] - sin_t * part[2],
            part[4],
            cos_t * part[5] + sin_t * part[6],
            cos_t * part[6] - sin_t * part[5],
            part[7],
        ],
        axis=0,
    )
    slots = turned.T
    for r in range(6):
        donors[pl.ds(r, 16, stride=8), :] = slots[16 * r : 16 * r + 16, :]
    base = 8 * lax.rem(source, 16)
    slot = iota((16, CP), 1)
    group = iota((16, CP), 0)
    named = jnp.where(lax.rem(slot, 16) == group, dest.astype(F32), 0.0)
    slot_down = iota((CP, CP), 0)
    placed = jnp.where(iota((CP, CP), 1) == base + slot_down // 16, 1.0, 0.0)
    donors[pl.ds(6, 16, stride=8), :] = jnp.dot(
        named, placed, preferred_element_type=F32, precision=lax.Precision.HIGHEST
    )
    donors[pl.ds(7, 16, stride=8), :] = jnp.zeros((16, CP), F32)


def route_kernel(
    dens, vel, mag, pres, row_in, col_in, weight_in, turn_in, dest_in,
    out_top, out_bottom, out_left, out_right,
    first_row, last_row, left_col, right_col, donors, ints, floats,
    top, bottom, left, right, slots, pieces, dense, inbox, total, handed,
    halo_send, halo_recv, donor_send, donor_recv, relay_send, relay_recv,
    dense_send, dense_recv, column_send, hand_send, hand_recv, pass_send,
):
    p = lax.axis_index("patch")
    z = lax.axis_index("theta")
    f = lax.axis_index("phi")
    on_row = (z == 0) | (z == NZ - 1)
    on_column = (f == 0) | (f == NF - 1)
    is_source = on_row | on_column
    column_hub = (z == HUBS[2]) | (z == HUBS[3])
    direct_hub = (z == HUBS[0]) | (z == HUBS[1]) | column_hub
    is_hub = direct_hub | (z == NZ - 1)
    half = z // 16
    hub_low = 16 * (z // 16)

    def partner(step):
        dx = sum(jnp.where(step == i, x, 0) for i, (x, _) in enumerate(STEPS))
        dy = sum(jnp.where(step == i, y, 0) for i, (_, y) in enumerate(STEPS))
        return 4 * lax.rem(f // 4 + dx, 4) + lax.rem(lax.rem(f, 4) + dy, 4)

    barrier = pltpu.get_barrier_semaphore()

    def greet(device):
        pl.semaphore_signal(barrier, inc=1, device_id=device, device_id_type=MESH)

    @pl.when(direct_hub)
    def _():
        @pl.loop(0, NZ // 2)
        def _(off):
            greet((p, lax.rem(z + NZ // 2 + off, NZ), f))

        @pl.loop(1, NZ // 2)
        def _(off):
            greet((p, lax.rem(z + off, NZ), f))

    @pl.when(z == NZ - 1)
    def _():
        greet((p, 0, f))

    @pl.when(z == 0)
    def _():
        greet((p, 1, f))

    @pl.when(is_hub)
    def _():
        @pl.loop(1, NF)
        def _(off):
            greet((p, z, lax.rem(f + off, NF)))

    @pl.when(on_row)
    def _():
        @pl.loop(0, NF)
        def _(j):
            greet((1 - p, z, j))

    @pl.when(jnp.logical_not(on_row))
    def _():
        greet((1 - p, z, 0))
        greet((1 - p, z, NF - 1))

    @pl.when(on_column)
    def _():
        greet((p, jnp.where(half == 0, HUBS[2], HUBS[3]), z - 16 * half))

    for has, device in (
        (z > 0, (p, z - 1, f)),
        (z < NZ - 1, (p, z + 1, f)),
        (f > 0, (p, z, f - 1)),
        (f < NF - 1, (p, z, f + 1)),
    ):
        pl.when(has)(functools.partial(greet, device))

    plane_low = jnp.where(z == 0, 0, jnp.where(z == NZ - 1, NF, 2 * NF + 2 * (z - 1)))
    source = plane_low + jnp.where(on_row, f, jnp.where(f == 0, 0, 1))
    comps = components(dens, vel, mag, pres)

    @pl.when(is_source)
    def _():
        find_donors(
            source, comps, row_in, col_in, weight_in, turn_in, dest_in, donors, ints, floats
        )

    @pl.when(is_hub)
    def _():
        slots[8 * SOURCES : SLOT_ROWS, :] = jnp.zeros((SLOT_ROWS - 8 * SOURCES, CP), F32)

    peers = (
        jnp.where(z > 0, 1, 0)
        + jnp.where(z < NZ - 1, 1, 0)
        + jnp.where(f > 0, 1, 0)
        + jnp.where(f < NF - 1, 1, 0)
        + jnp.where(direct_hub, 3, 4)
        + jnp.where(is_hub, NF - 1, 0)
        + jnp.where(column_hub, 2, 0)
        + jnp.where((z == 0) | (z == 1), 1, 0)
        + jnp.where(is_source, NF, 0)
    )
    pl.semaphore_wait(barrier, peers)

    def halo(which):
        src, dst, device = (
            (last_row, top, (p, z + 1, f)),
            (first_row, bottom, (p, z - 1, f)),
            (right_col, left, (p, z, f + 1)),
            (left_col, right, (p, z, f - 1)),
        )[which]
        return pltpu.make_async_remote_copy(
            src_ref=src,
            dst_ref=dst,
            send_sem=halo_send.at[which],
            recv_sem=halo_recv.at[which],
            device_id=device,
            device_id_type=MESH,
        )

    sends_to = (z < NZ - 1, z > 0, f < NF - 1, f > 0)
    hears_from = (z > 0, z < NZ - 1, f > 0, f < NF - 1)

    @pl.when(is_source)
    def _():
        @pl.loop(0, NF)
        def _(step):
            j = partner(step)
            pltpu.make_async_remote_copy(
                src_ref=donors.at[pl.ds(pl.multiple_of(8 * j, 8), 8)],
                dst_ref=slots.at[pl.ds(pl.multiple_of(8 * source, 8), 8)],
                send_sem=donor_send,
                recv_sem=donor_recv,
                device_id=(1 - p, z, j),
                device_id_type=MESH,
            ).start()

    pack(comps, first_row, last_row, left_col, right_col)
    for which in range(4):

        @pl.when(sends_to[which])
        def _():
            halo(which).start()

    def whole_wait(ref, sem):
        return pltpu.make_async_copy(ref, ref, sem).wait()

    def relay(tiles, hub):
        rows = slots.at[pl.ds(pl.multiple_of(8 * plane_low, 8), 8 * tiles)]
        return pltpu.make_async_remote_copy(
            src_ref=rows,
            dst_ref=rows,
            send_sem=relay_send.at[hub],
            recv_sem=relay_recv,
            device_id=(p, HUBS[hub], f),
            device_id_type=MESH,
        )

    for here, tiles in ((on_row, NF), (jnp.logical_not(on_row), 2)):

        @pl.when(here)
        def _():
            whole_wait(slots.at[pl.ds(0, 8 * tiles)], donor_recv)
            for hub in range(4):

                @pl.when(z != HUBS[hub])
                def _():
                    relay(tiles, hub).start()

    def split_slots():
        value = slots[...]
        high = value.astype(BF16)
        rest = value - high.astype(F32)
        mid = rest.astype(BF16)
        pieces[:, 0:CP] = high
        pieces[:, CP : 2 * CP] = mid
        pieces[:, 2 * CP :] = (rest - mid.astype(F32)).astype(BF16)
        ids = slots[pl.ds(6, 96, stride=8), :]
        return jnp.concatenate(
            [jnp.sum(ids[16 * g : 16 * g + 16, :], axis=0, keepdims=True) for g in range(6)],
            axis=1,
        )

    def place(ids, wanted):
        hits = jnp.where(ids == wanted.astype(F32), 1.0, 0.0).astype(BF16)
        out = jnp.dot(hits, pieces[...], preferred_element_type=F32)
        return out[:, 0:CP] + out[:, CP : 2 * CP] + out[:, 2 * CP :]

    point = iota((CP, 1), 0)

    def block_copy(rows, j):
        return pltpu.make_async_remote_copy(
            src_ref=dense.at[pl.ds(pl.multiple_of(rows * j, rows), rows)],
            dst_ref=inbox.at[pl.ds(pl.multiple_of(rows * f, rows), rows)],
            send_sem=dense_send,
            recv_sem=dense_recv,
            device_id=(p, z, j),
            device_id_type=MESH,
        )

    def gather_blocks(rows):
        whole_wait(inbox.at[pl.ds(0, rows * (NF - 1))], dense_recv)
        own = dense[pl.ds(pl.multiple_of(rows * f, rows), rows), :]

        def step(off, acc):
            j = lax.rem(f + off, NF)
            return acc + inbox[pl.ds(pl.multiple_of(rows * j, rows), rows), :]

        return lax.fori_loop(1, NF, step, own)

    def exchange(rows, first):
        ids = split_slots()
        points = iota((rows, 1), 0)

        @pl.loop(0, NF)
        def _(step):
            j = partner(step)
            dense[pl.ds(pl.multiple_of(rows * j, rows), rows), :] = place(
                ids, first + CP * j + points
            )

            @pl.when(step > 0)
            def _():
                block_copy(rows, partner(step - 1)).start()

        return gather_blocks(rows)

    def exchange_done(rows):
        whole_wait(dense.at[pl.ds(0, rows * (NF - 1))], dense_send)

    def hand_over():
        return pltpu.make_async_remote_copy(
            src_ref=total,
            dst_ref=handed,
            send_sem=hand_send,
            recv_sem=hand_recv,
            device_id=(p, 0, f),
            device_id_type=MESH,
        )

    def pass_on(which):
        low, count = ((0, NF), (2 * NF, SOURCES - 2 * NF))[which]
        rows = slots.at[pl.ds(8 * low, 8 * count)]
        return pltpu.make_async_remote_copy(
            src_ref=rows,
            dst_ref=rows,
            send_sem=pass_send.at[which],
            recv_sem=relay_recv,
            device_id=(p, NZ - 1, f),
            device_id_type=MESH,
        )

    @pl.when(z == 0)
    def _():
        whole_wait(slots.at[pl.ds(0, 8 * (SOURCES - NF))], relay_recv)
        pass_on(0).start()
        pass_on(1).start()
        border = exchange(TOP_ROWS[0], 1)
        whole_wait(handed, hand_recv)
        top[...] = jnp.concatenate([border, handed[...]], axis=0).T
        exchange_done(TOP_ROWS[0])
        pass_on(0).wait_send()
        pass_on(1).wait_send()

    @pl.when(z == 1)
    def _():
        whole_wait(slots.at[pl.ds(0, 8 * (SOURCES - 2))], relay_recv)
        total[...] = exchange(TOP_ROWS[1], 1 + TOP_ROWS[0])
        exchange_done(TOP_ROWS[1])
        hand_over().start()
        hand_over().wait_send()

    @pl.when(z == NZ - 1)
    def _():
        whole_wait(slots.at[pl.ds(0, 8 * (SOURCES - NF))], relay_recv)
        bottom[...] = exchange(CP, 1 + NPH).T
        exchange_done(CP)

    @pl.when(column_hub)
    def _():
        whole_wait(slots.at[pl.ds(0, 8 * (SOURCES - 2))], relay_recv)
        ids = split_slots()
        side = lax.rem(point, 32) // 16
        first = 1 + 2 * NPH + NTH * side + lax.rem(point, 16) + CT * (hub_low + point // 32)

        @pl.loop(0, 4)
        def _(quad):
            dense[pl.ds(pl.multiple_of(CP * quad, CP), CP), :] = place(ids, first + CT * 4 * quad)

        @pl.loop(0, NF - 1)
        def _(step):
            block_copy(32, partner(step)).start()

        total[0:32, :] = gather_blocks(32)
        whole_wait(dense.at[pl.ds(0, 32 * (NF - 1))], dense_send)

        def forward(side_of, dst):
            return pltpu.make_async_remote_copy(
                src_ref=total.at[pl.ds(16 * side_of, 16)],
                dst_ref=dst,
                send_sem=column_send.at[side_of],
                recv_sem=halo_recv.at[2 + side_of],
                device_id=(p, hub_low + f, (NF - 1) * side_of),
                device_id_type=MESH,
            )

        copies = [forward(0, left), forward(1, right)]
        for copy in copies:
            copy.start()
        for copy in copies:
            copy.wait_send()

    for which, ref in enumerate((top, bottom)):

        @pl.when(hears_from[which])
        def _():
            whole_wait(ref, halo_recv.at[which])

    for which, ref in ((2, left), (3, right)):
        whole_wait(ref, halo_recv.at[which])

    out_top[...] = top[...]
    out_bottom[...] = bottom[...]
    out_left[...] = left[...]
    out_right[...] = right[...]

    for which in range(4):

        @pl.when(sends_to[which])
        def _():
            halo(which).wait_send()

    @pl.when(is_source)
    def _():
        whole_wait(donors, donor_send)

    for here, tiles in ((on_row, NF), (jnp.logical_not(on_row), 2)):
        for hub in range(4):

            @pl.when(here & (z != HUBS[hub]))
            def _():
                relay(tiles, hub).wait_send()


def step_kernel(
    constants, dens, vel, mag, pres, top, bottom, left, right,
    new_dens, new_vel, new_mag, new_pres,
):
    d_theta, d_phi, dt, nu = constants
    z = lax.axis_index("theta")
    comps = components(dens, vel, mag, pres)
    row = iota((CT, CP), 0)
    lane = iota((CT, CP), 1)
    angle = 0.25 * math.pi + ((z * CT + row).astype(F32) + 0.5) * d_theta
    inv_sin = 1.0 / jnp.sin(angle)
    inv_sin_sq = inv_sin * inv_sin
    left_all, right_all = left[...], right[...]
    gr = 1.0 / DR_STEP

    for k in range(NR):
        radius = R_BASE + (k + 0.5) * DR_STEP
        gt = 1.0 / (radius * d_theta)
        gp = 1.0 / (radius * d_phi)
        hr, ht, hp = 0.5 * gr, 0.5 * gt, (0.5 * gp) * inv_sin
        lr, lt, lp = nu * gr * gr, nu * gt * gt, (nu * gp * gp) * inv_sin_sq
        C, U, D, N, S, W, E = ([], [], [], [], [], [], [])
        for c in range(8):
            ck = c * NR + k
            here = comps[c][k]
            C.append(here)
            U.append(comps[c][min(k + 1, NR - 1)])
            D.append(comps[c][max(k - 1, 0)])
            N.append(jnp.where(row == 0, top[ck : ck + 1, :], pltpu.roll(here, 1, 0)))
            S.append(jnp.where(row == CT - 1, bottom[ck : ck + 1, :], pltpu.roll(here, CT - 1, 0)))
            shift_w, shift_e = (CP - ck) % CP, (CP - 1 - ck) % CP
            edge_w = pltpu.roll(left_all, shift_w, 1) if shift_w else left_all
            edge_e = pltpu.roll(right_all, shift_e, 1) if shift_e else right_all
            W.append(jnp.where(lane == 0, edge_w, pltpu.roll(here, 1, 1)))
            E.append(jnp.where(lane == CP - 1, edge_e, pltpu.roll(here, CP - 1, 1)))

        def dr(c):
            return (U[c] - D[c]) * hr

        def dt_(c):
            return (S[c] - N[c]) * ht

        def dp(c):
            return (E[c] - W[c]) * hp

        def laplace(c):
            twice = 2.0 * C[c]
            return (
                (U[c] + D[c] - twice) * lr
                + (S[c] + N[c] - twice) * lt
                + (E[c] + W[c] - twice) * lp
            )

        def emf(side, comp):
            a, b = (((2, 6), (3, 5)), ((3, 4), (1, 6)), ((1, 5), (2, 4)))[comp]
            return side[a[0]] * side[a[1]] - side[b[0]] * side[b[1]]

        rho, p = C[0], C[7]
        v = C[1:4]
        b = C[4:7]
        grad_v = [(dr(c), dt_(c), dp(c)) for c in (1, 2, 3)]
        grad_p = (dr(7), dt_(7), dp(7))
        div_mom = (
            (U[0] * U[1] - D[0] * D[1]) * hr
            + (S[0] * S[2] - N[0] * N[2]) * ht
            + (E[0] * E[3] - W[0] * W[3]) * hp
        )
        new_dens[k] = rho - dt * div_mom
        j_r = dt_(6) - dp(5)
        j_t = dp(4) - dr(6)
        j_p = dr(5) - dt_(4)
        force = (j_t * b[2] - j_p * b[1], j_p * b[0] - j_r * b[2], j_r * b[1] - j_t * b[0])
        inv_rho = 1.0 / rho

        def carried(grad):
            return v[0] * grad[0] + v[1] * grad[1] + v[2] * grad[2]

        for c in range(3):
            new_vel[c, k] = v[c] + dt * (
                (force[c] - grad_p[c]) * inv_rho - carried(grad_v[c]) + laplace(1 + c)
            )
        div_v = grad_v[0][0] + grad_v[1][1] + grad_v[2][2]
        new_pres[k] = p + dt * (laplace(7) - carried(grad_p) - GAMMA * p * div_v)
        dt_ep = (emf(S, 2) - emf(N, 2)) * ht
        dp_et = (emf(E, 1) - emf(W, 1)) * hp
        dp_er = (emf(E, 0) - emf(W, 0)) * hp
        dr_ep = (emf(U, 2) - emf(D, 2)) * hr
        dr_et = (emf(U, 1) - emf(D, 1)) * hr
        dt_er = (emf(S, 0) - emf(N, 0)) * ht
        new_mag[0, k] = b[0] + dt * (dt_ep - dp_et + laplace(4))
        new_mag[1, k] = b[1] + dt * (dp_er - dr_ep + laplace(5))
        new_mag[2, k] = b[2] + dt * (dr_et - dt_er + laplace(6))


VMEM = pl.BlockSpec(memory_space=pltpu.VMEM)


def shape(*dims):
    return jax.ShapeDtypeStruct(dims, F32)


def body(
    density, velocity, magnetic, pressure, send_row, send_col, send_weight, send_turn, send_dest
):
    fields = (density[0], velocity[0], magnetic[0], pressure[0])
    halos = pl.pallas_call(
        route_kernel,
        out_shape=(shape(CH, CP), shape(CH, CP), shape(CT, CP), shape(CT, CP)),
        in_specs=[VMEM] * 9,
        out_specs=(VMEM,) * 4,
        scratch_shapes=[
            pltpu.VMEM((CH, CP), F32),
            pltpu.VMEM((CH, CP), F32),
            pltpu.VMEM((CT, CP), F32),
            pltpu.VMEM((CT, CP), F32),
            pltpu.VMEM((CP, CP), F32),
            pltpu.VMEM((8, CP), jnp.int32),
            pltpu.VMEM((8, CP), F32),
            pltpu.VMEM((CH, CP), F32),
            pltpu.VMEM((CH, CP), F32),
            pltpu.VMEM((CT, CP), F32),
            pltpu.VMEM((CT, CP), F32),
            pltpu.VMEM((SLOT_ROWS, CP), F32),
            pltpu.VMEM((SLOT_ROWS, 3 * CP), BF16),
            pltpu.VMEM((NF * CP, CP), F32),
            pltpu.VMEM((NF * CP, CP), F32),
            pltpu.VMEM((TOP_ROWS[1], CP), F32),
            pltpu.VMEM((TOP_ROWS[1], CP), F32),
            pltpu.SemaphoreType.DMA((4,)),
            pltpu.SemaphoreType.DMA((4,)),
            pltpu.SemaphoreType.DMA,
            pltpu.SemaphoreType.DMA,
            pltpu.SemaphoreType.DMA((4,)),
            pltpu.SemaphoreType.DMA,
            pltpu.SemaphoreType.DMA,
            pltpu.SemaphoreType.DMA,
            pltpu.SemaphoreType.DMA((2,)),
            pltpu.SemaphoreType.DMA,
            pltpu.SemaphoreType.DMA,
            pltpu.SemaphoreType.DMA((2,)),
        ],
        compiler_params=pltpu.CompilerParams(collective_id=0, has_side_effects=True),
        name="route",
    )(
        *fields,
        send_row.reshape(1, SEND),
        send_col.reshape(1, SEND),
        send_weight.reshape(2, SEND),
        send_turn.reshape(1, SEND),
        send_dest.reshape(1, SEND),
    )
    new_density, new_flow, new_magnet, new_press = pl.pallas_call(
        functools.partial(step_kernel, grid_constants(NTH, NPH)),
        out_shape=(shape(NR, CT, CP), shape(3, NR, CT, CP), shape(3, NR, CT, CP), shape(NR, CT, CP)),
        in_specs=[VMEM] * 8,
        out_specs=(VMEM,) * 4,
        name="step",
    )(*fields, *halos)
    return (new_density[None], new_flow[None], new_magnet[None], new_press[None])


def solution(mesh):
    return jax.shard_map(
        body,
        mesh=mesh,
        in_specs=(
            P("patch", None, "theta", "phi"),
            P("patch", None, None, "theta", "phi"),
            P("patch", None, None, "theta", "phi"),
            P("patch", None, "theta", "phi"),
            P("patch", "theta", "phi", None),
            P("patch", "theta", "phi", None),
            P("patch", "theta", "phi", None, None),
            P("patch", "theta", "phi", None),
            P("patch", "theta", "phi", None),
        ),
        out_specs=(
            P("patch", None, "theta", "phi"),
            P("patch", None, None, "theta", "phi"),
            P("patch", None, None, "theta", "phi"),
            P("patch", None, "theta", "phi"),
        ),
        check_vma=False,
    )
```

```python
import functools
import math

import jax
import jax.numpy as jnp
from jax import lax
from jax.experimental import pallas as pl
from jax.experimental.pallas import tpu as pltpu
from jax.sharding import PartitionSpec as P

MESH = pl.DeviceIdType.MESH
F32 = jnp.float32
BF16 = jnp.bfloat16

GAMMA = 5.0 / 3.0
R_BASE = 0.6
DR_STEP = 0.65 / 64.0
COURANT = 0.4
DIFFUSE = 0.4

NR, CT, CP = 16, 16, 128
NZ, NF = 32, 16
NPH, NTH = CP * NF, CT * NZ
SEND = 96
CH = 8 * NR
LOW, HIGH = 1, 20
TILE, CARRIED = 16, 12
GROUPS = NF // 2
STEPS = (
    (2, 2), (2, 1), (1, 2), (2, 3), (3, 2), (1, 1), (3, 3), (1, 3), (3, 1),
    (2, 0), (0, 2), (1, 0), (0, 1), (3, 0), (0, 3),
)
SOURCES = 2 * NF + 2 * (NZ - 2)
SLOT_ROWS = 96 * 16


def grid_constants(total_theta, total_phi):
    d_theta = 0.5 * math.pi / total_theta
    d_phi = 1.5 * math.pi / total_phi
    r_low = R_BASE + 0.5 * DR_STEP
    inv_r = 1.0 / DR_STEP
    inv_t = 1.0 / (r_low * d_theta)
    inv_p = 1.0 / (r_low * math.sin(0.25 * math.pi) * d_phi)
    dt_step = COURANT / (inv_r + inv_t + inv_p)
    diffusivity = DIFFUSE / (dt_step * (inv_r * inv_r + inv_t * inv_t + inv_p * inv_p))
    return (d_theta, d_phi, dt_step, diffusivity)


def components(dens, vel, mag, pres):
    return [dens, vel.at[0], vel.at[1], vel.at[2], mag.at[0], mag.at[1], mag.at[2], pres]


def iota(shape, dim):
    return lax.broadcasted_iota(jnp.int32, shape, dim)


def pack(comps, first_row, last_row, left_col, right_col):
    for c in range(8):
        first_row[c * NR : (c + 1) * NR, :] = comps[c][:, 0, :]
        last_row[c * NR : (c + 1) * NR, :] = comps[c][:, CT - 1, :]
    lane = iota((CT, CP), 1)
    low = jnp.zeros((CT, CP), F32)
    high = jnp.zeros((CT, CP), F32)
    for c in range(8):
        for k in range(NR):
            ck = c * NR + k
            block = comps[c][k]
            low = jnp.where(lane == ck, pltpu.roll(block, ck, 1) if ck else block, low)
            shift = (ck + 1) % CP
            high = jnp.where(lane == ck, pltpu.roll(block, shift, 1) if shift else block, high)
    left_col[...] = low
    right_col[...] = high


def find_donors(source, comps, row_in, col_in, weight_in, turn_in, dest_in, donors, ints, floats):
    ints[...] = jnp.zeros_like(ints)
    floats[...] = jnp.zeros_like(floats)
    ints[0:1, 0:SEND] = row_in[...]
    ints[1:2, 0:SEND] = col_in[...]
    ints[2:3, 0:SEND] = jnp.where(dest_in[...] < 2 * (NPH + NTH), dest_in[...] + 1, 0)
    floats[0:2, 0:SEND] = weight_in[...]
    floats[2:3, 0:SEND] = turn_in[...]
    row, col, dest = ints[0:1, :], ints[1:2, :], ints[2:3, :]
    weight_row, weight_col, turn = floats[0:1, :], floats[1:2, :], floats[2:3, :]
    cell = iota((CP, CP), 0)
    col_mix = jnp.where(cell == col, 1.0 - weight_col, 0.0) + jnp.where(
        cell == col + 1, weight_col, 0.0
    )
    level = iota((CT, CP), 0)
    row_mix = jnp.where(level == row, 1.0 - weight_row, 0.0) + jnp.where(
        level == row + 1, weight_row, 0.0
    )
    value = jnp.zeros((CH, CP), F32)
    for i in range(CT):
        line = jnp.concatenate([comps[c][:, i, :] for c in range(8)], axis=0)
        mixed = jnp.dot(
            line, col_mix, preferred_element_type=F32, precision=lax.Precision.HIGHEST
        )
        value = value + row_mix[i : i + 1, :] * mixed
    cos_t, sin_t = jnp.cos(turn), jnp.sin(turn)
    part = [value[c * NR : (c + 1) * NR, :] for c in range(8)]
    turned = jnp.concatenate(
        [
            part[0],
            part[1],
            cos_t * part[2] + sin_t * part[3],
            cos_t * part[3] - sin_t * part[2],
            part[4],
            cos_t * part[5] + sin_t * part[6],
            cos_t * part[6] - sin_t * part[5],
            part[7],
        ],
        axis=0,
    )
    slots = turned.T
    for r in range(CARRIED):
        donors[pl.ds(r, GROUPS, stride=TILE), :] = slots[GROUPS * r : GROUPS * (r + 1), :]
    base = TILE * lax.rem(source, 8)
    slot = iota((GROUPS, CP), 1)
    group = iota((GROUPS, CP), 0)
    named = jnp.where(lax.rem(slot, GROUPS) == group, dest.astype(F32), 0.0)
    slot_down = iota((CP, CP), 0)
    placed = jnp.where(iota((CP, CP), 1) == base + slot_down // GROUPS, 1.0, 0.0)
    donors[pl.ds(CARRIED, GROUPS, stride=TILE), :] = jnp.dot(
        named, placed, preferred_element_type=F32, precision=lax.Precision.HIGHEST
    )
    for r in range(CARRIED + 1, TILE):
        donors[pl.ds(r, GROUPS, stride=TILE), :] = jnp.zeros((GROUPS, CP), F32)


def route_kernel(
    dens, vel, mag, pres, row_in, col_in, weight_in, turn_in, dest_in,
    out_top, out_bottom, out_left, out_right,
    first_row, last_row, left_col, right_col, donors, ints, floats,
    top, bottom, left, right, slots, pieces, dense, inbox, total,
    halo_send, halo_recv, donor_send, donor_recv, relay_send, relay_recv,
    dense_send, dense_recv, column_send, pass_send,
):
    p = lax.axis_index("patch")
    z = lax.axis_index("theta")
    f = lax.axis_index("phi")
    on_row = (z == 0) | (z == NZ - 1)
    on_column = (f == 0) | (f == NF - 1)
    is_source = on_row | on_column
    odd = lax.rem(f // 4 + lax.rem(f, 4), 2)
    even = odd == 0
    serves_columns = (z == LOW) | (z == HIGH)
    row_hub = on_row & even
    column_hub = serves_columns & (odd == 1)
    half = z // 16
    hub_low = 16 * half

    def partner(step):
        dx = sum(jnp.where(step == i, x, 0) for i, (x, _) in enumerate(STEPS))
        dy = sum(jnp.where(step == i, y, 0) for i, (_, y) in enumerate(STEPS))
        return 4 * lax.rem(f // 4 + dx, 4) + lax.rem(lax.rem(f, 4) + dy, 4)

    barrier = pltpu.get_barrier_semaphore()

    def greet(device):
        pl.semaphore_signal(barrier, inc=1, device_id=device, device_id_type=MESH)

    @pl.when(((z == 0) & even) | column_hub)
    def _():
        @pl.loop(0, NZ // 2)
        def _(off):
            greet((p, lax.rem(z + NZ // 2 + off, NZ), f))

        @pl.loop(1, NZ // 2)
        def _(off):
            greet((p, lax.rem(z + off, NZ), f))

    @pl.when((z == NZ - 1) & even)
    def _():
        greet((p, 0, f))

    def greet_parity(which):
        @pl.loop(0, GROUPS)
        def _(g):
            turn = lax.rem(g // 2, 2)
            j = 2 * g + (turn if which == 0 else 1 - turn)

            @pl.when(j != f)
            def _():
                greet((p, z, j))

    pl.when(on_row)(functools.partial(greet_parity, 0))
    pl.when(serves_columns)(functools.partial(greet_parity, 1))

    @pl.when(on_row)
    def _():
        @pl.loop(0, NF)
        def _(j):
            greet((1 - p, z, j))

    @pl.when(jnp.logical_not(on_row))
    def _():
        greet((1 - p, z, 0))
        greet((1 - p, z, NF - 1))

    @pl.when(on_column)
    def _():
        greet((p, jnp.where(half == 0, LOW, HIGH), z - 16 * half))

    for has, device in (
        (z > 0, (p, z - 1, f)),
        (z < NZ - 1, (p, z + 1, f)),
        (f > 0, (p, z, f - 1)),
        (f < NF - 1, (p, z, f + 1)),
    ):
        pl.when(has)(functools.partial(greet, device))

    plane_low = jnp.where(z == 0, 0, jnp.where(z == NZ - 1, NF, 2 * NF + 2 * (z - 1)))
    source = plane_low + jnp.where(on_row, f, jnp.where(f == 0, 0, 1))
    comps = components(dens, vel, mag, pres)

    @pl.when(is_source)
    def _():
        find_donors(
            source, comps, row_in, col_in, weight_in, turn_in, dest_in, donors, ints, floats
        )

    @pl.when(row_hub | column_hub)
    def _():
        slots[TILE * SOURCES : SLOT_ROWS, :] = jnp.zeros((SLOT_ROWS - TILE * SOURCES, CP), F32)

    peers = (
        jnp.where(z > 0, 1, 0)
        + jnp.where(z < NZ - 1, 1, 0)
        + jnp.where(f > 0, 1, 0)
        + jnp.where(f < NF - 1, 1, 0)
        + jnp.where(even, jnp.where(z != 0, 1, 0), jnp.where(serves_columns, 1, 2))
        + jnp.where(row_hub | column_hub, NF - 1, 0)
        + jnp.where(serves_columns, 2, 0)
        + jnp.where((z == 0) & even, 1, 0)
        + jnp.where(is_source, NF, 0)
    )
    pl.semaphore_wait(barrier, peers)

    def halo(which):
        src, dst, device = (
            (last_row, top, (p, z + 1, f)),
            (first_row, bottom, (p, z - 1, f)),
            (right_col, left, (p, z, f + 1)),
            (left_col, right, (p, z, f - 1)),
        )[which]
        return pltpu.make_async_remote_copy(
            src_ref=src,
            dst_ref=dst,
            send_sem=halo_send.at[which],
            recv_sem=halo_recv.at[which],
            device_id=device,
            device_id_type=MESH,
        )

    sends_to = (z < NZ - 1, z > 0, f < NF - 1, f > 0)
    hears_from = (z > 0, z < NZ - 1, f > 0, f < NF - 1)

    @pl.when(is_source)
    def _():
        @pl.loop(0, NF)
        def _(step):
            j = partner(step)
            pltpu.make_async_remote_copy(
                src_ref=donors.at[pl.ds(pl.multiple_of(TILE * (j // 2), TILE), TILE)],
                dst_ref=slots.at[pl.ds(pl.multiple_of(TILE * source, TILE), TILE)],
                send_sem=donor_send,
                recv_sem=donor_recv,
                device_id=(1 - p, z, j),
                device_id_type=MESH,
            ).start()

    pack(comps, first_row, last_row, left_col, right_col)
    for which in range(4):

        @pl.when(sends_to[which])
        def _():
            halo(which).start()

    def whole_wait(ref, sem):
        return pltpu.make_async_copy(ref, ref, sem).wait()

    PLANES = (0, LOW, HIGH)
    goes = (even & (z != 0), (odd == 1) & (z != LOW), (odd == 1) & (z != HIGH))

    def relay(tiles, to):
        rows = slots.at[pl.ds(pl.multiple_of(TILE * plane_low, TILE), TILE * tiles)]
        return pltpu.make_async_remote_copy(
            src_ref=rows,
            dst_ref=rows,
            send_sem=relay_send.at[to],
            recv_sem=relay_recv,
            device_id=(p, PLANES[to], f),
            device_id_type=MESH,
        )

    for here, tiles in ((on_row, NF), (jnp.logical_not(on_row), 2)):

        @pl.when(here)
        def _():
            whole_wait(slots.at[pl.ds(0, TILE * tiles)], donor_recv)
            for to in range(3):

                @pl.when(goes[to])
                def _():
                    relay(tiles, to).start()

    def split_slots():
        value = slots[...]
        high = value.astype(BF16)
        rest = value - high.astype(F32)
        mid = rest.astype(BF16)
        pieces[:, 0:CP] = high
        pieces[:, CP : 2 * CP] = mid
        pieces[:, 2 * CP :] = (rest - mid.astype(F32)).astype(BF16)
        ids = slots[pl.ds(CARRIED, 96, stride=TILE), :]
        return jnp.concatenate(
            [jnp.sum(ids[8 * g : 8 * g + 8, :], axis=0, keepdims=True) for g in range(12)],
            axis=1,
        )

    def place(ids, wanted):
        hits = jnp.where(ids == wanted.astype(F32), 1.0, 0.0).astype(BF16)
        out = jnp.dot(hits, pieces[...], preferred_element_type=F32)
        return out[:, 0:CP] + out[:, CP : 2 * CP] + out[:, 2 * CP :]

    def block_copy(rows, j):
        return pltpu.make_async_remote_copy(
            src_ref=dense.at[pl.ds(pl.multiple_of(rows * j, rows), rows)],
            dst_ref=inbox.at[pl.ds(pl.multiple_of(rows * (f // 2), rows), rows)],
            send_sem=dense_send,
            recv_sem=dense_recv,
            device_id=(p, z, j),
            device_id_type=MESH,
        )

    def keep_own(rows):
        mine = dense[pl.ds(pl.multiple_of(rows * f, rows), rows), :]
        inbox[pl.ds(pl.multiple_of(rows * (f // 2), rows), rows), :] = mine

    def gather_blocks(rows):
        for has, count in ((even, GROUPS - 1), (odd == 1, GROUPS)):
            if rows != CP:
                count = 2 * GROUPS - 1 - count

            @pl.when(has)
            def _():
                whole_wait(inbox.at[pl.ds(0, rows * count)], dense_recv)

        total = inbox[0:rows, :]
        for g in range(1, GROUPS):
            total = total + inbox[rows * g : rows * (g + 1), :]
        return total

    def exchange(first):
        ids = split_slots()
        point = iota((2 * CP, 1), 0)

        @pl.loop(0, GROUPS)
        def _(step):
            one, two = partner(2 * step), partner(2 * step + 1)
            wanted = first + point + jnp.where(point < CP, CP * one, CP * two - CP)
            blocks = place(ids, wanted)
            dense[pl.ds(pl.multiple_of(CP * one, CP), CP), :] = blocks[:CP]
            dense[pl.ds(pl.multiple_of(CP * two, CP), CP), :] = blocks[CP:]

            @pl.when(step > 0)
            def _():
                block_copy(CP, partner(2 * step - 2)).start()
                block_copy(CP, partner(2 * step - 1)).start()

        keep_own(CP)
        block_copy(CP, partner(NF - 2)).start()

    def pass_on(which):
        low, count = ((0, NF), (2 * NF, SOURCES - 2 * NF))[which]
        rows = slots.at[pl.ds(TILE * low, TILE * count)]
        return pltpu.make_async_remote_copy(
            src_ref=rows,
            dst_ref=rows,
            send_sem=pass_send.at[which],
            recv_sem=relay_recv,
            device_id=(p, NZ - 1, f),
            device_id_type=MESH,
        )

    def forward(side):
        return pltpu.make_async_remote_copy(
            src_ref=total.at[pl.ds(CT * side, CT)],
            dst_ref=(left, right)[side],
            send_sem=column_send.at[side],
            recv_sem=halo_recv.at[2 + side],
            device_id=(p, hub_low + f, (NF - 1) * side),
            device_id_type=MESH,
        )

    @pl.when(row_hub)
    def _():
        whole_wait(slots.at[pl.ds(0, TILE * (SOURCES - NF))], relay_recv)

        @pl.when(z == 0)
        def _():
            pass_on(0).start()
            pass_on(1).start()

        exchange(1 + jnp.where(z == 0, 0, NPH))

    @pl.when(z == 0)
    def _():
        top[...] = gather_blocks(CP).T

    @pl.when(z == NZ - 1)
    def _():
        bottom[...] = gather_blocks(CP).T

    @pl.when(column_hub)
    def _():
        whole_wait(slots.at[pl.ds(0, TILE * (SOURCES - 2))], relay_recv)
        ids = split_slots()
        point = iota((CP, 1), 0)
        side = lax.rem(point, 32) // 16
        first = 1 + 2 * NPH + NTH * side + lax.rem(point, 16) + CT * (hub_low + point // 32)

        @pl.loop(0, 4)
        def _(quad):
            dense[pl.ds(pl.multiple_of(CP * quad, CP), CP), :] = place(ids, first + CT * 4 * quad)

        keep_own(2 * CT)

        @pl.loop(0, NF - 1)
        def _(step):
            block_copy(2 * CT, partner(step)).start()

    @pl.when(serves_columns)
    def _():
        total[...] = gather_blocks(2 * CT)
        copies = [forward(0), forward(1)]
        for copy in copies:
            copy.start()
        for copy in copies:
            copy.wait_send()

    for which, ref in enumerate((top, bottom)):

        @pl.when(hears_from[which])
        def _():
            whole_wait(ref, halo_recv.at[which])

    for which, ref in ((2, left), (3, right)):
        whole_wait(ref, halo_recv.at[which])

    out_top[...] = top[...]
    out_bottom[...] = bottom[...]
    out_left[...] = left[...]
    out_right[...] = right[...]

    for which in range(4):

        @pl.when(sends_to[which])
        def _():
            halo(which).wait_send()

    @pl.when(is_source)
    def _():
        whole_wait(slots.at[pl.ds(0, TILE * NF)], donor_send)

    for here, tiles in ((on_row, NF), (jnp.logical_not(on_row), 2)):
        for to in range(3):

            @pl.when(here & goes[to])
            def _():
                relay(tiles, to).wait_send()

    @pl.when(row_hub)
    def _():
        whole_wait(dense.at[pl.ds(0, CP * (NF - 1))], dense_send)

    @pl.when(column_hub)
    def _():
        whole_wait(dense.at[pl.ds(0, 2 * CT * (NF - 1))], dense_send)

    @pl.when((z == 0) & even)
    def _():
        pass_on(0).wait_send()
        pass_on(1).wait_send()


def step_kernel(
    constants, dens, vel, mag, pres, top, bottom, left, right,
    new_dens, new_vel, new_mag, new_pres,
):
    d_theta, d_phi, dt, nu = constants
    z = lax.axis_index("theta")
    comps = components(dens, vel, mag, pres)
    row = iota((CT, CP), 0)
    lane = iota((CT, CP), 1)
    angle = 0.25 * math.pi + ((z * CT + row).astype(F32) + 0.5) * d_theta
    inv_sin = 1.0 / jnp.sin(angle)
    inv_sin_sq = inv_sin * inv_sin
    left_all, right_all = left[...], right[...]
    gr = 1.0 / DR_STEP

    for k in range(NR):
        radius = R_BASE + (k + 0.5) * DR_STEP
        gt = 1.0 / (radius * d_theta)
        gp = 1.0 / (radius * d_phi)
        hr, ht, hp = 0.5 * gr, 0.5 * gt, (0.5 * gp) * inv_sin
        lr, lt, lp = nu * gr * gr, nu * gt * gt, (nu * gp * gp) * inv_sin_sq
        C, U, D, N, S, W, E = ([], [], [], [], [], [], [])
        for c in range(8):
            ck = c * NR + k
            here = comps[c][k]
            C.append(here)
            U.append(comps[c][min(k + 1, NR - 1)])
            D.append(comps[c][max(k - 1, 0)])
            N.append(jnp.where(row == 0, top[ck : ck + 1, :], pltpu.roll(here, 1, 0)))
            S.append(jnp.where(row == CT - 1, bottom[ck : ck + 1, :], pltpu.roll(here, CT - 1, 0)))
            shift_w, shift_e = (CP - ck) % CP, (CP - 1 - ck) % CP
            edge_w = pltpu.roll(left_all, shift_w, 1) if shift_w else left_all
            edge_e = pltpu.roll(right_all, shift_e, 1) if shift_e else right_all
            W.append(jnp.where(lane == 0, edge_w, pltpu.roll(here, 1, 1)))
            E.append(jnp.where(lane == CP - 1, edge_e, pltpu.roll(here, CP - 1, 1)))

        def dr(c):
            return (U[c] - D[c]) * hr

        def dt_(c):
            return (S[c] - N[c]) * ht

        def dp(c):
            return (E[c] - W[c]) * hp

        def laplace(c):
            twice = 2.0 * C[c]
            return (
                (U[c] + D[c] - twice) * lr
                + (S[c] + N[c] - twice) * lt
                + (E[c] + W[c] - twice) * lp
            )

        def emf(side, comp):
            a, b = (((2, 6), (3, 5)), ((3, 4), (1, 6)), ((1, 5), (2, 4)))[comp]
            return side[a[0]] * side[a[1]] - side[b[0]] * side[b[1]]

        rho, p = C[0], C[7]
        v = C[1:4]
        b = C[4:7]
        grad_v = [(dr(c), dt_(c), dp(c)) for c in (1, 2, 3)]
        grad_p = (dr(7), dt_(7), dp(7))
        div_mom = (
            (U[0] * U[1] - D[0] * D[1]) * hr
            + (S[0] * S[2] - N[0] * N[2]) * ht
            + (E[0] * E[3] - W[0] * W[3]) * hp
        )
        new_dens[k] = rho - dt * div_mom
        j_r = dt_(6) - dp(5)
        j_t = dp(4) - dr(6)
        j_p = dr(5) - dt_(4)
        force = (j_t * b[2] - j_p * b[1], j_p * b[0] - j_r * b[2], j_r * b[1] - j_t * b[0])
        inv_rho = 1.0 / rho

        def carried(grad):
            return v[0] * grad[0] + v[1] * grad[1] + v[2] * grad[2]

        for c in range(3):
            new_vel[c, k] = v[c] + dt * (
                (force[c] - grad_p[c]) * inv_rho - carried(grad_v[c]) + laplace(1 + c)
            )
        div_v = grad_v[0][0] + grad_v[1][1] + grad_v[2][2]
        new_pres[k] = p + dt * (laplace(7) - carried(grad_p) - GAMMA * p * div_v)
        dt_ep = (emf(S, 2) - emf(N, 2)) * ht
        dp_et = (emf(E, 1) - emf(W, 1)) * hp
        dp_er = (emf(E, 0) - emf(W, 0)) * hp
        dr_ep = (emf(U, 2) - emf(D, 2)) * hr
        dr_et = (emf(U, 1) - emf(D, 1)) * hr
        dt_er = (emf(S, 0) - emf(N, 0)) * ht
        new_mag[0, k] = b[0] + dt * (dt_ep - dp_et + laplace(4))
        new_mag[1, k] = b[1] + dt * (dp_er - dr_ep + laplace(5))
        new_mag[2, k] = b[2] + dt * (dr_et - dt_er + laplace(6))


VMEM = pl.BlockSpec(memory_space=pltpu.VMEM)


def shape(*dims):
    return jax.ShapeDtypeStruct(dims, F32)


def body(
    density, velocity, magnetic, pressure, send_row, send_col, send_weight, send_turn, send_dest
):
    fields = (density[0], velocity[0], magnetic[0], pressure[0])
    halos = pl.pallas_call(
        route_kernel,
        out_shape=(shape(CH, CP), shape(CH, CP), shape(CT, CP), shape(CT, CP)),
        in_specs=[VMEM] * 9,
        out_specs=(VMEM,) * 4,
        scratch_shapes=[
            pltpu.VMEM((CH, CP), F32),
            pltpu.VMEM((CH, CP), F32),
            pltpu.VMEM((CT, CP), F32),
            pltpu.VMEM((CT, CP), F32),
            pltpu.VMEM((CP, CP), F32),
            pltpu.VMEM((8, CP), jnp.int32),
            pltpu.VMEM((8, CP), F32),
            pltpu.VMEM((CH, CP), F32),
            pltpu.VMEM((CH, CP), F32),
            pltpu.VMEM((CT, CP), F32),
            pltpu.VMEM((CT, CP), F32),
            pltpu.VMEM((SLOT_ROWS, CP), F32),
            pltpu.VMEM((SLOT_ROWS, 3 * CP), BF16),
            pltpu.VMEM((NF * CP, CP), F32),
            pltpu.VMEM((GROUPS * CP, CP), F32),
            pltpu.VMEM((2 * CT, CP), F32),
            pltpu.SemaphoreType.DMA((4,)),
            pltpu.SemaphoreType.DMA((4,)),
            pltpu.SemaphoreType.DMA,
            pltpu.SemaphoreType.DMA,
            pltpu.SemaphoreType.DMA((3,)),
            pltpu.SemaphoreType.DMA,
            pltpu.SemaphoreType.DMA,
            pltpu.SemaphoreType.DMA,
            pltpu.SemaphoreType.DMA((2,)),
            pltpu.SemaphoreType.DMA((2,)),
        ],
        compiler_params=pltpu.CompilerParams(collective_id=0, has_side_effects=True),
        name="route",
    )(
        *fields,
        send_row.reshape(1, SEND),
        send_col.reshape(1, SEND),
        send_weight.reshape(2, SEND),
        send_turn.reshape(1, SEND),
        send_dest.reshape(1, SEND),
    )
    new_density, new_flow, new_magnet, new_press = pl.pallas_call(
        functools.partial(step_kernel, grid_constants(NTH, NPH)),
        out_shape=(shape(NR, CT, CP), shape(3, NR, CT, CP), shape(3, NR, CT, CP), shape(NR, CT, CP)),
        in_specs=[VMEM] * 8,
        out_specs=(VMEM,) * 4,
        name="step",
    )(*fields, *halos)
    return (new_density[None], new_flow[None], new_magnet[None], new_press[None])


def solution(mesh):
    return jax.shard_map(
        body,
        mesh=mesh,
        in_specs=(
            P("patch", None, "theta", "phi"),
            P("patch", None, None, "theta", "phi"),
            P("patch", None, None, "theta", "phi"),
            P("patch", None, "theta", "phi"),
            P("patch", "theta", "phi", None),
            P("patch", "theta", "phi", None),
            P("patch", "theta", "phi", None, None),
            P("patch", "theta", "phi", None),
            P("patch", "theta", "phi", None),
        ),
        out_specs=(
            P("patch", None, "theta", "phi"),
            P("patch", None, None, "theta", "phi"),
            P("patch", None, None, "theta", "phi"),
            P("patch", None, "theta", "phi"),
        ),
        check_vma=False,
    )
```

```python
import functools
import math

import jax
import jax.numpy as jnp
from jax import lax
from jax.experimental import pallas as pl
from jax.experimental.pallas import tpu as pltpu
from jax.sharding import PartitionSpec as P

MESH = pl.DeviceIdType.MESH
F32 = jnp.float32
BF16 = jnp.bfloat16

GAMMA = 5.0 / 3.0
R_BASE = 0.6
DR_STEP = 0.65 / 64.0
COURANT = 0.4
DIFFUSE = 0.4

NR, CT, CP = 16, 16, 128
NZ, NF = 32, 16
NPH, NTH = CP * NF, CT * NZ
SEND = 96
CH = 8 * NR
HIGH = 20
BLOCK = 80
EVEN_CHIPS = (0, 2, 5, 7, 8, 10, 13, 15)
ODD_CHIPS = (1, 3, 4, 6, 9, 11, 12, 14)
TILE, CARRIED = 16, 12
GROUPS = NF // 2
STEPS = (
    (2, 2), (2, 1), (1, 2), (2, 3), (3, 2), (1, 1), (3, 3), (1, 3), (3, 1),
    (2, 0), (0, 2), (1, 0), (0, 1), (3, 0), (0, 3),
)
SOURCES = 2 * NF + 2 * (NZ - 2)
SLOT_ROWS = 96 * 16


def grid_constants(total_theta, total_phi):
    d_theta = 0.5 * math.pi / total_theta
    d_phi = 1.5 * math.pi / total_phi
    r_low = R_BASE + 0.5 * DR_STEP
    inv_r = 1.0 / DR_STEP
    inv_t = 1.0 / (r_low * d_theta)
    inv_p = 1.0 / (r_low * math.sin(0.25 * math.pi) * d_phi)
    dt_step = COURANT / (inv_r + inv_t + inv_p)
    diffusivity = DIFFUSE / (dt_step * (inv_r * inv_r + inv_t * inv_t + inv_p * inv_p))
    return (d_theta, d_phi, dt_step, diffusivity)


def components(dens, vel, mag, pres):
    return [dens, vel.at[0], vel.at[1], vel.at[2], mag.at[0], mag.at[1], mag.at[2], pres]


def iota(shape, dim):
    return lax.broadcasted_iota(jnp.int32, shape, dim)


def pack(comps, first_row, last_row, left_col, right_col):
    for c in range(8):
        first_row[c * NR : (c + 1) * NR, :] = comps[c][:, 0, :]
        last_row[c * NR : (c + 1) * NR, :] = comps[c][:, CT - 1, :]
    lane = iota((CT, CP), 1)
    low = jnp.zeros((CT, CP), F32)
    high = jnp.zeros((CT, CP), F32)
    for c in range(8):
        for k in range(NR):
            ck = c * NR + k
            block = comps[c][k]
            low = jnp.where(lane == ck, pltpu.roll(block, ck, 1) if ck else block, low)
            shift = (ck + 1) % CP
            high = jnp.where(lane == ck, pltpu.roll(block, shift, 1) if shift else block, high)
    left_col[...] = low
    right_col[...] = high


def find_donors(source, comps, row_in, col_in, weight_in, turn_in, dest_in, donors, ints, floats):
    ints[...] = jnp.zeros_like(ints)
    floats[...] = jnp.zeros_like(floats)
    ints[0:1, 0:SEND] = row_in[...]
    ints[1:2, 0:SEND] = col_in[...]
    ints[2:3, 0:SEND] = jnp.where(dest_in[...] < 2 * (NPH + NTH), dest_in[...] + 1, 0)
    floats[0:2, 0:SEND] = weight_in[...]
    floats[2:3, 0:SEND] = turn_in[...]
    row, col, dest = ints[0:1, :], ints[1:2, :], ints[2:3, :]
    weight_row, weight_col, turn = floats[0:1, :], floats[1:2, :], floats[2:3, :]
    cell = iota((CP, CP), 0)
    col_mix = jnp.where(cell == col, 1.0 - weight_col, 0.0) + jnp.where(
        cell == col + 1, weight_col, 0.0
    )
    level = iota((CT, CP), 0)
    row_mix = jnp.where(level == row, 1.0 - weight_row, 0.0) + jnp.where(
        level == row + 1, weight_row, 0.0
    )
    value = jnp.zeros((CH, CP), F32)
    for i in range(CT):
        line = jnp.concatenate([comps[c][:, i, :] for c in range(8)], axis=0)
        mixed = jnp.dot(
            line, col_mix, preferred_element_type=F32, precision=lax.Precision.HIGHEST
        )
        value = value + row_mix[i : i + 1, :] * mixed
    cos_t, sin_t = jnp.cos(turn), jnp.sin(turn)
    part = [value[c * NR : (c + 1) * NR, :] for c in range(8)]
    turned = jnp.concatenate(
        [
            part[0],
            part[1],
            cos_t * part[2] + sin_t * part[3],
            cos_t * part[3] - sin_t * part[2],
            part[4],
            cos_t * part[5] + sin_t * part[6],
            cos_t * part[6] - sin_t * part[5],
            part[7],
        ],
        axis=0,
    )
    slots = turned.T
    for r in range(CARRIED):
        donors[pl.ds(r, GROUPS, stride=TILE), :] = slots[GROUPS * r : GROUPS * (r + 1), :]
    base = TILE * lax.rem(source, 8)
    slot = iota((GROUPS, CP), 1)
    group = iota((GROUPS, CP), 0)
    named = jnp.where(lax.rem(slot, GROUPS) == group, dest.astype(F32), 0.0)
    slot_down = iota((CP, CP), 0)
    placed = jnp.where(iota((CP, CP), 1) == base + slot_down // GROUPS, 1.0, 0.0)
    donors[pl.ds(CARRIED, GROUPS, stride=TILE), :] = jnp.dot(
        named, placed, preferred_element_type=F32, precision=lax.Precision.HIGHEST
    )
    for r in range(CARRIED + 1, TILE):
        donors[pl.ds(r, GROUPS, stride=TILE), :] = jnp.zeros((GROUPS, CP), F32)


def route_kernel(
    dens, vel, mag, pres, row_in, col_in, weight_in, turn_in, dest_in,
    out_top, out_bottom, out_left, out_right,
    first_row, last_row, left_col, right_col, donors, ints, floats,
    top, bottom, left, right, slots, pieces, dense, inbox, total,
    halo_send, halo_recv, donor_send, donor_recv, relay_send, relay_recv,
    dense_send, dense_recv, column_send, pass_send,
):
    p = lax.axis_index("patch")
    z = lax.axis_index("theta")
    f = lax.axis_index("phi")
    on_row = (z == 0) | (z == NZ - 1)
    on_column = (f == 0) | (f == NF - 1)
    is_source = on_row | on_column
    odd = lax.rem(f // 4 + lax.rem(f, 4), 2)
    even = odd == 0
    column_hub = (z == HIGH) & (odd == 1)
    at_home = (z == 0) & (f == 0)
    half = z // 16
    hub_low = 16 * half

    def partner(step):
        dx = sum(jnp.where(step == i, x, 0) for i, (x, _) in enumerate(STEPS))
        dy = sum(jnp.where(step == i, y, 0) for i, (_, y) in enumerate(STEPS))
        return 4 * lax.rem(f // 4 + dx, 4) + lax.rem(lax.rem(f, 4) + dy, 4)

    barrier = pltpu.get_barrier_semaphore()

    def greet(device):
        pl.semaphore_signal(barrier, inc=1, device_id=device, device_id_type=MESH)

    @pl.when((z == 0) | column_hub)
    def _():
        @pl.loop(0, NZ // 2)
        def _(off):
            greet((p, lax.rem(z + NZ // 2 + off, NZ), f))

        @pl.loop(1, NZ // 2)
        def _(off):
            greet((p, lax.rem(z + off, NZ), f))

    @pl.when(z == NZ - 1)
    def _():
        greet((p, 0, f))

    @pl.when(on_row)
    def _():
        @pl.loop(1, NF)
        def _(off):
            greet((p, z, lax.rem(f + off, NF)))

    @pl.when(z == HIGH)
    def _():
        @pl.loop(0, GROUPS)
        def _(g):
            j = 2 * g + 1 - lax.rem(g // 2, 2)

            @pl.when(j != f)
            def _():
                greet((p, z, j))

    @pl.when(on_row)
    def _():
        @pl.loop(0, NF)
        def _(j):
            greet((1 - p, z, j))

    @pl.when(jnp.logical_not(on_row))
    def _():
        greet((1 - p, z, 0))
        greet((1 - p, z, NF - 1))

    @pl.when(on_column & jnp.logical_not(at_home))
    def _():
        greet((p, HIGH * half, z - 16 * half))

    for has, device in (
        (z > 0, (p, z - 1, f)),
        (z < NZ - 1, (p, z + 1, f)),
        (f > 0, (p, z, f - 1)),
        (f < NF - 1, (p, z, f + 1)),
    ):
        pl.when(has)(functools.partial(greet, device))

    plane_low = jnp.where(z == 0, 0, jnp.where(z == NZ - 1, NF, 2 * NF + 2 * (z - 1)))
    source = plane_low + jnp.where(on_row, f, jnp.where(f == 0, 0, 1))
    comps = components(dens, vel, mag, pres)

    @pl.when(is_source)
    def _():
        find_donors(
            source, comps, row_in, col_in, weight_in, turn_in, dest_in, donors, ints, floats
        )

    @pl.when(on_row | column_hub)
    def _():
        slots[TILE * SOURCES : SLOT_ROWS, :] = jnp.zeros((SLOT_ROWS - TILE * SOURCES, CP), F32)

    peers = (
        jnp.where(z > 0, 1, 0)
        + jnp.where(z < NZ - 1, 1, 0)
        + jnp.where(f > 0, 1, 0)
        + jnp.where(f < NF - 1, 1, 0)
        + jnp.where(z != 0, 1, 2)
        + jnp.where((odd == 1) & (z != HIGH), 1, 0)
        + jnp.where(on_row | column_hub, NF - 1, 0)
        + jnp.where(z == HIGH, 2, 0)
        + jnp.where(z == 0, jnp.where(f == 0, 0, 1), 0)
        + jnp.where(is_source, NF, 0)
    )
    pl.semaphore_wait(barrier, peers)

    def halo(which):
        src, dst, device = (
            (last_row, top, (p, z + 1, f)),
            (first_row, bottom, (p, z - 1, f)),
            (right_col, left, (p, z, f + 1)),
            (left_col, right, (p, z, f - 1)),
        )[which]
        return pltpu.make_async_remote_copy(
            src_ref=src,
            dst_ref=dst,
            send_sem=halo_send.at[which],
            recv_sem=halo_recv.at[which],
            device_id=device,
            device_id_type=MESH,
        )

    sends_to = (z < NZ - 1, z > 0, f < NF - 1, f > 0)
    hears_from = (z > 0, z < NZ - 1, f > 0, f < NF - 1)

    @pl.when(is_source)
    def _():
        @pl.loop(0, NF)
        def _(step):
            j = partner(step)
            pltpu.make_async_remote_copy(
                src_ref=donors.at[pl.ds(pl.multiple_of(TILE * (j // 2), TILE), TILE)],
                dst_ref=slots.at[pl.ds(pl.multiple_of(TILE * source, TILE), TILE)],
                send_sem=donor_send,
                recv_sem=donor_recv,
                device_id=(1 - p, z, j),
                device_id_type=MESH,
            ).start()

    pack(comps, first_row, last_row, left_col, right_col)
    for which in range(4):

        @pl.when(sends_to[which])
        def _():
            halo(which).start()

    def whole_wait(ref, sem):
        return pltpu.make_async_copy(ref, ref, sem).wait()

    PLANES = (0, HIGH)
    goes = (z != 0, (odd == 1) & (z != HIGH))

    def relay(tiles, to):
        rows = slots.at[pl.ds(pl.multiple_of(TILE * plane_low, TILE), TILE * tiles)]
        return pltpu.make_async_remote_copy(
            src_ref=rows,
            dst_ref=rows,
            send_sem=relay_send.at[to],
            recv_sem=relay_recv,
            device_id=(p, PLANES[to], f),
            device_id_type=MESH,
        )

    for here, tiles in ((on_row, NF), (jnp.logical_not(on_row), 2)):

        @pl.when(here)
        def _():
            whole_wait(slots.at[pl.ds(0, TILE * tiles)], donor_recv)
            for to in range(2):

                @pl.when(goes[to])
                def _():
                    relay(tiles, to).start()

    def split_slots():
        value = slots[...]
        high = value.astype(BF16)
        rest = value - high.astype(F32)
        mid = rest.astype(BF16)
        pieces[:, 0:CP] = high
        pieces[:, CP : 2 * CP] = mid
        pieces[:, 2 * CP :] = (rest - mid.astype(F32)).astype(BF16)
        ids = slots[pl.ds(CARRIED, 96, stride=TILE), :]
        return jnp.concatenate(
            [jnp.sum(ids[8 * g : 8 * g + 8, :], axis=0, keepdims=True) for g in range(12)],
            axis=1,
        )

    def place(ids, wanted):
        hits = jnp.where(ids == wanted.astype(F32), 1.0, 0.0).astype(BF16)
        out = jnp.dot(hits, pieces[...], preferred_element_type=F32)
        return out[:, 0:CP] + out[:, CP : 2 * CP] + out[:, 2 * CP :]

    def inbox_of(rows):
        place_in = rows * (f if rows == BLOCK else f // 2)
        return inbox.at[pl.ds(pl.multiple_of(place_in, 16), rows)]

    def block_copy(rows, j):
        return pltpu.make_async_remote_copy(
            src_ref=dense.at[pl.ds(pl.multiple_of(rows * j, rows), rows)],
            dst_ref=inbox_of(rows),
            send_sem=dense_send,
            recv_sem=dense_recv,
            device_id=(p, z, j),
            device_id_type=MESH,
        )

    def keep_own(rows):
        mine = dense[pl.ds(pl.multiple_of(rows * f, rows), rows), :]
        inbox_of(rows)[...] = mine

    def sum_of(rows, places):
        out = inbox[rows * places[0] : rows * (places[0] + 1), :]
        for g in places[1:]:
            out = out + inbox[rows * g : rows * (g + 1), :]
        return out

    def exchange():
        ids = split_slots()
        row = iota((2 * BLOCK, 1), 0)
        second = row >= BLOCK
        t = jnp.where(second, row - BLOCK, row)
        first = 1 + jnp.where(z == 0, 0, NPH)
        after = t - (CP - BLOCK)
        column = 1 + 2 * NPH + jnp.where(after < CT, after, NTH + after - CT)

        @pl.loop(0, GROUPS)
        def _(step):
            one, two = partner(2 * step), partner(2 * step + 1)
            j = jnp.where(second, two, one)
            in_row = first + CP * j + t
            last = jnp.where(
                after < 0, in_row + BLOCK, jnp.where(z == 0, column + CT * j, -1)
            )
            blocks = place(ids, jnp.where(even, in_row, last))
            dense[pl.ds(pl.multiple_of(BLOCK * one, BLOCK), BLOCK), :] = blocks[:BLOCK]
            dense[pl.ds(pl.multiple_of(BLOCK * two, BLOCK), BLOCK), :] = blocks[BLOCK:]

            @pl.when(step > 0)
            def _():
                block_copy(BLOCK, partner(2 * step - 2)).start()
                block_copy(BLOCK, partner(2 * step - 1)).start()

        keep_own(BLOCK)
        block_copy(BLOCK, partner(NF - 2)).start()

    def pass_on(which):
        low, count = ((0, NF), (2 * NF, SOURCES - 2 * NF))[which]
        rows = slots.at[pl.ds(TILE * low, TILE * count)]
        return pltpu.make_async_remote_copy(
            src_ref=rows,
            dst_ref=rows,
            send_sem=pass_send.at[which],
            recv_sem=relay_recv,
            device_id=(p, NZ - 1, f),
            device_id_type=MESH,
        )

    def forward(side):
        return pltpu.make_async_remote_copy(
            src_ref=total.at[pl.ds(CT * side, CT)],
            dst_ref=(left, right)[side],
            send_sem=column_send.at[side],
            recv_sem=halo_recv.at[2 + side],
            device_id=(p, hub_low + f, (NF - 1) * side),
            device_id_type=MESH,
        )

    @pl.when(on_row)
    def _():
        whole_wait(slots.at[pl.ds(0, TILE * (SOURCES - NF))], relay_recv)

        @pl.when(z == 0)
        def _():
            pass_on(0).start()
            pass_on(1).start()

        exchange()
        whole_wait(inbox.at[pl.ds(0, BLOCK * (NF - 1))], dense_recv)
        rest = sum_of(BLOCK, ODD_CHIPS)
        total[...] = rest[CP - BLOCK :]
        border = jnp.concatenate([sum_of(BLOCK, EVEN_CHIPS), rest[: CP - BLOCK]], axis=0).T

        @pl.when(z == 0)
        def _():
            @pl.when(f == 0)
            def _():
                left[...] = total[0:CT, :]

            @pl.when(f != 0)
            def _():
                forward(0).start()

            forward(1).start()
            top[...] = border

        @pl.when(z == NZ - 1)
        def _():
            bottom[...] = border

    @pl.when(column_hub)
    def _():
        whole_wait(slots.at[pl.ds(0, TILE * (SOURCES - 2))], relay_recv)
        ids = split_slots()
        point = iota((CP, 1), 0)
        side = lax.rem(point, 32) // 16
        first = 1 + 2 * NPH + NTH * side + lax.rem(point, 16) + CT * (hub_low + point // 32)

        @pl.loop(0, 4)
        def _(quad):
            dense[pl.ds(pl.multiple_of(CP * quad, CP), CP), :] = place(ids, first + CT * 4 * quad)

        keep_own(2 * CT)

        @pl.loop(0, NF - 1)
        def _(step):
            block_copy(2 * CT, partner(step)).start()

    @pl.when(z == HIGH)
    def _():
        for has, count in ((even, GROUPS), (odd == 1, GROUPS - 1)):

            @pl.when(has)
            def _():
                whole_wait(inbox.at[pl.ds(0, 2 * CT * count)], dense_recv)

        total[...] = sum_of(2 * CT, tuple(range(GROUPS)))
        forward(0).start()
        forward(1).start()

    for which, ref in enumerate((top, bottom)):

        @pl.when(hears_from[which])
        def _():
            whole_wait(ref, halo_recv.at[which])

    @pl.when(jnp.logical_not(at_home))
    def _():
        whole_wait(left, halo_recv.at[2])

    whole_wait(right, halo_recv.at[3])

    out_top[...] = top[...]
    out_bottom[...] = bottom[...]
    out_left[...] = left[...]
    out_right[...] = right[...]

    for which in range(4):

        @pl.when(sends_to[which])
        def _():
            halo(which).wait_send()

    @pl.when(is_source)
    def _():
        whole_wait(slots.at[pl.ds(0, TILE * NF)], donor_send)

    for here, tiles in ((on_row, NF), (jnp.logical_not(on_row), 2)):
        for to in range(2):

            @pl.when(here & goes[to])
            def _():
                relay(tiles, to).wait_send()

    @pl.when(on_row)
    def _():
        whole_wait(dense.at[pl.ds(0, BLOCK * (NF - 1))], dense_send)

    @pl.when(column_hub)
    def _():
        whole_wait(dense.at[pl.ds(0, 2 * CT * (NF - 1))], dense_send)

    @pl.when(((z == 0) & (f != 0)) | (z == HIGH))
    def _():
        forward(0).wait_send()

    @pl.when((z == 0) | (z == HIGH))
    def _():
        forward(1).wait_send()

    @pl.when(z == 0)
    def _():
        pass_on(0).wait_send()
        pass_on(1).wait_send()


def step_kernel(
    constants, dens, vel, mag, pres, top, bottom, left, right,
    new_dens, new_vel, new_mag, new_pres,
):
    d_theta, d_phi, dt, nu = constants
    z = lax.axis_index("theta")
    comps = components(dens, vel, mag, pres)
    row = iota((CT, CP), 0)
    lane = iota((CT, CP), 1)
    angle = 0.25 * math.pi + ((z * CT + row).astype(F32) + 0.5) * d_theta
    inv_sin = 1.0 / jnp.sin(angle)
    inv_sin_sq = inv_sin * inv_sin
    left_all, right_all = left[...], right[...]
    gr = 1.0 / DR_STEP

    for k in range(NR):
        radius = R_BASE + (k + 0.5) * DR_STEP
        gt = 1.0 / (radius * d_theta)
        gp = 1.0 / (radius * d_phi)
        hr, ht, hp = 0.5 * gr, 0.5 * gt, (0.5 * gp) * inv_sin
        lr, lt, lp = nu * gr * gr, nu * gt * gt, (nu * gp * gp) * inv_sin_sq
        C, U, D, N, S, W, E = ([], [], [], [], [], [], [])
        for c in range(8):
            ck = c * NR + k
            here = comps[c][k]
            C.append(here)
            U.append(comps[c][min(k + 1, NR - 1)])
            D.append(comps[c][max(k - 1, 0)])
            N.append(jnp.where(row == 0, top[ck : ck + 1, :], pltpu.roll(here, 1, 0)))
            S.append(jnp.where(row == CT - 1, bottom[ck : ck + 1, :], pltpu.roll(here, CT - 1, 0)))
            shift_w, shift_e = (CP - ck) % CP, (CP - 1 - ck) % CP
            edge_w = pltpu.roll(left_all, shift_w, 1) if shift_w else left_all
            edge_e = pltpu.roll(right_all, shift_e, 1) if shift_e else right_all
            W.append(jnp.where(lane == 0, edge_w, pltpu.roll(here, 1, 1)))
            E.append(jnp.where(lane == CP - 1, edge_e, pltpu.roll(here, CP - 1, 1)))

        def dr(c):
            return (U[c] - D[c]) * hr

        def dt_(c):
            return (S[c] - N[c]) * ht

        def dp(c):
            return (E[c] - W[c]) * hp

        def laplace(c):
            twice = 2.0 * C[c]
            return (
                (U[c] + D[c] - twice) * lr
                + (S[c] + N[c] - twice) * lt
                + (E[c] + W[c] - twice) * lp
            )

        def emf(side, comp):
            a, b = (((2, 6), (3, 5)), ((3, 4), (1, 6)), ((1, 5), (2, 4)))[comp]
            return side[a[0]] * side[a[1]] - side[b[0]] * side[b[1]]

        rho, p = C[0], C[7]
        v = C[1:4]
        b = C[4:7]
        grad_v = [(dr(c), dt_(c), dp(c)) for c in (1, 2, 3)]
        grad_p = (dr(7), dt_(7), dp(7))
        div_mom = (
            (U[0] * U[1] - D[0] * D[1]) * hr
            + (S[0] * S[2] - N[0] * N[2]) * ht
            + (E[0] * E[3] - W[0] * W[3]) * hp
        )
        new_dens[k] = rho - dt * div_mom
        j_r = dt_(6) - dp(5)
        j_t = dp(4) - dr(6)
        j_p = dr(5) - dt_(4)
        force = (j_t * b[2] - j_p * b[1], j_p * b[0] - j_r * b[2], j_r * b[1] - j_t * b[0])
        inv_rho = 1.0 / rho

        def carried(grad):
            return v[0] * grad[0] + v[1] * grad[1] + v[2] * grad[2]

        for c in range(3):
            new_vel[c, k] = v[c] + dt * (
                (force[c] - grad_p[c]) * inv_rho - carried(grad_v[c]) + laplace(1 + c)
            )
        div_v = grad_v[0][0] + grad_v[1][1] + grad_v[2][2]
        new_pres[k] = p + dt * (laplace(7) - carried(grad_p) - GAMMA * p * div_v)
        dt_ep = (emf(S, 2) - emf(N, 2)) * ht
        dp_et = (emf(E, 1) - emf(W, 1)) * hp
        dp_er = (emf(E, 0) - emf(W, 0)) * hp
        dr_ep = (emf(U, 2) - emf(D, 2)) * hr
        dr_et = (emf(U, 1) - emf(D, 1)) * hr
        dt_er = (emf(S, 0) - emf(N, 0)) * ht
        new_mag[0, k] = b[0] + dt * (dt_ep - dp_et + laplace(4))
        new_mag[1, k] = b[1] + dt * (dp_er - dr_ep + laplace(5))
        new_mag[2, k] = b[2] + dt * (dr_et - dt_er + laplace(6))


VMEM = pl.BlockSpec(memory_space=pltpu.VMEM)


def shape(*dims):
    return jax.ShapeDtypeStruct(dims, F32)


def body(
    density, velocity, magnetic, pressure, send_row, send_col, send_weight, send_turn, send_dest
):
    fields = (density[0], velocity[0], magnetic[0], pressure[0])
    halos = pl.pallas_call(
        route_kernel,
        out_shape=(shape(CH, CP), shape(CH, CP), shape(CT, CP), shape(CT, CP)),
        in_specs=[VMEM] * 9,
        out_specs=(VMEM,) * 4,
        scratch_shapes=[
            pltpu.VMEM((CH, CP), F32),
            pltpu.VMEM((CH, CP), F32),
            pltpu.VMEM((CT, CP), F32),
            pltpu.VMEM((CT, CP), F32),
            pltpu.VMEM((CP, CP), F32),
            pltpu.VMEM((8, CP), jnp.int32),
            pltpu.VMEM((8, CP), F32),
            pltpu.VMEM((CH, CP), F32),
            pltpu.VMEM((CH, CP), F32),
            pltpu.VMEM((CT, CP), F32),
            pltpu.VMEM((CT, CP), F32),
            pltpu.VMEM((SLOT_ROWS, CP), F32),
            pltpu.VMEM((SLOT_ROWS, 3 * CP), BF16),
            pltpu.VMEM((NF * CP, CP), F32),
            pltpu.VMEM((NF * BLOCK, CP), F32),
            pltpu.VMEM((2 * CT, CP), F32),
            pltpu.SemaphoreType.DMA((4,)),
            pltpu.SemaphoreType.DMA((4,)),
            pltpu.SemaphoreType.DMA,
            pltpu.SemaphoreType.DMA,
            pltpu.SemaphoreType.DMA((3,)),
            pltpu.SemaphoreType.DMA,
            pltpu.SemaphoreType.DMA,
            pltpu.SemaphoreType.DMA,
            pltpu.SemaphoreType.DMA((2,)),
            pltpu.SemaphoreType.DMA((2,)),
        ],
        compiler_params=pltpu.CompilerParams(collective_id=0, has_side_effects=True),
        name="route",
    )(
        *fields,
        send_row.reshape(1, SEND),
        send_col.reshape(1, SEND),
        send_weight.reshape(2, SEND),
        send_turn.reshape(1, SEND),
        send_dest.reshape(1, SEND),
    )
    new_density, new_flow, new_magnet, new_press = pl.pallas_call(
        functools.partial(step_kernel, grid_constants(NTH, NPH)),
        out_shape=(shape(NR, CT, CP), shape(3, NR, CT, CP), shape(3, NR, CT, CP), shape(NR, CT, CP)),
        in_specs=[VMEM] * 8,
        out_specs=(VMEM,) * 4,
        name="step",
    )(*fields, *halos)
    return (new_density[None], new_flow[None], new_magnet[None], new_press[None])


def solution(mesh):
    return jax.shard_map(
        body,
        mesh=mesh,
        in_specs=(
            P("patch", None, "theta", "phi"),
            P("patch", None, None, "theta", "phi"),
            P("patch", None, None, "theta", "phi"),
            P("patch", None, "theta", "phi"),
            P("patch", "theta", "phi", None),
            P("patch", "theta", "phi", None),
            P("patch", "theta", "phi", None, None),
            P("patch", "theta", "phi", None),
            P("patch", "theta", "phi", None),
        ),
        out_specs=(
            P("patch", None, "theta", "phi"),
            P("patch", None, None, "theta", "phi"),
            P("patch", None, None, "theta", "phi"),
            P("patch", None, "theta", "phi"),
        ),
        check_vma=False,
    )
```
